32 devices in a mesh: ma: 4 (over x, core), ell: 8 (over z, y).
Axes of the slice: x: 2, y: 2, z: 4, core: 2. Of those that a mesh axis runs over, the one named last changes fastest.
Arguments:
- legendre: bfloat16 [3, 2048, 2, 4096], P(None, 'ma', None, 'ell'), may hold values from -6 to 6
- harmonics: bfloat16 [2048, 3, 2, 4, 4096], P('ma', None, None, None, 'ell'), may hold values from -0.0014648438 to 0.0014648438
- slot_orders: int32 [2048], replicated, may hold values from 0 to 2047, each once
- cycle_index: int32 [2], replicated, may hold values from 2048 to 4095
Outputs:
- maps: float32 [4, 3, 4, 8192], P('ma', None, None, 'ell')
The draws below stay inside these ranges and needn't reach their ends.
Inputs may be any that keep to these rules, and one draw needn't show every extreme that they name: `slot_orders`: every number from 0 to 2047 appears once.
All inputs are finite; a program needn't handle non-finite values.
Results may differ from the reference program's by a relative error of at most 0.0003.
Values sent between devices are 32-bit elements; how exact they have to be, the bound alone decides.
A program may use at most 128 MiB of HBM per device.

```python
import math
import jax
import jax.numpy as jnp
from jax import lax

L = 4096
COMPS = 4
SLOTS = 2048
NPIX = 8192
RPAIRS = 2


def steps_of(rng, extent, pieces, low, largest):
    factor_of, own = 1.0, jax.random.fold_in(rng, 6)
    for axis_at, parts in pieces:
        heights = jnp.exp(jax.random.uniform(jax.random.fold_in(own, axis_at), (parts,), jnp.float32, low / len(pieces), largest / len(pieces)))
        factor_of = factor_of * jnp.repeat(heights, extent[axis_at] // parts).reshape([-1 if axis == axis_at else 1 for axis in range(len(extent))])
    return factor_of


def gaussian(own_key, shape, width, most, pieces=(), held_as=jnp.bfloat16):
    factor_of = steps_of(own_key, shape, pieces, -0.22, 0.18) if pieces else 1.0
    result = jax.random.normal(own_key, shape, jnp.float32) * width * factor_of
    return jnp.minimum(jnp.maximum(result, -most), most).astype(held_as)


def setup_inputs(seed: int = 0) -> dict:
    splits = jax.random.split(jax.random.key(seed), 5)
    legendre = gaussian(splits[0], (3, SLOTS, RPAIRS, L), 1.0, 6.0, ((1, 4), (3, 8)))
    harmonics = gaussian(splits[1], (SLOTS, 3, 2, COMPS, L), (L * L) ** -0.5, 0.0014648438, ((0, 4), (4, 8)))
    slot_orders = jax.random.permutation(splits[2], SLOTS).astype(jnp.int32)
    cycle_index = jax.random.randint(splits[3], (RPAIRS,), L // 2, L).astype(jnp.int32)
    return dict(legendre=legendre, harmonics=harmonics, slot_orders=slot_orders, cycle_index=cycle_index)


def column_weights(lower_order, first_column, columns_count, full_width):
    columns = first_column + jnp.arange(columns_count, dtype=jnp.int32)
    boundary = (full_width - 1 - lower_order)[:, None]
    lower_part = (columns[None, :] < boundary).astype(jnp.float32)
    upper_part = ((columns[None, :] >= boundary) & (columns[None, :] < full_width - 1)).astype(jnp.float32)
    lower_sign = (1 - 2 * (columns[None, :] % 2)).astype(jnp.float32)
    upper_sign = (1 - 2 * ((columns[None, :] + 1 + lower_order[:, None]) % 2)).astype(jnp.float32)
    return jnp.stack([lower_part, lower_part * lower_sign, upper_part, upper_part * upper_sign], axis=1)


def spin_fields(plain, plus, minus):
    hemisphere = jnp.array([1.0, -1.0], jnp.float32).reshape(1, 1, 1, 2, 1, 1, 1)
    minus = minus * hemisphere
    temp_real = plain[:, :, :, :, 0]
    temp_imag = plain[:, :, :, :, 1]
    eplus_real = plus[:, :, :, :, 0, 0]
    eplus_imag = plus[:, :, :, :, 0, 1]
    bplus_real = plus[:, :, :, :, 1, 0]
    bplus_imag = plus[:, :, :, :, 1, 1]
    eminus_real = minus[:, :, :, :, 0, 0]
    eminus_imag = minus[:, :, :, :, 0, 1]
    bminus_real = minus[:, :, :, :, 1, 0]
    bminus_imag = minus[:, :, :, :, 1, 1]
    stokes_q_real = -(eplus_real - bminus_imag)
    stokes_q_imag = -(eplus_imag + bminus_real)
    stokes_u_real = -(bplus_real + eminus_imag)
    stokes_u_imag = -(bplus_imag - eminus_real)
    return jnp.stack([jnp.stack([temp_real, temp_imag]), jnp.stack([stokes_q_real, stokes_q_imag]), jnp.stack([stokes_u_real, stokes_u_imag])])


def reference(legendre, harmonics, slot_orders, cycle_index):
    highest = lax.Precision.HIGHEST
    block = min(16, SLOTS)

    def one_block(index):
        start = index * block
        tables = lax.dynamic_slice_in_dim(legendre, start, block, 1).astype(jnp.float32)
        coeffs = lax.dynamic_slice_in_dim(harmonics, start, block, 0).astype(jnp.float32)
        lower_order = lax.dynamic_slice_in_dim(slot_orders, start, block, 0)
        weights = column_weights(lower_order, 0, L, L)
        packed = coeffs[:, None] * weights[:, :, None, None, None, :]
        plain = jnp.einsum('srj,sqpcj->srqpc', tables[0], packed[:, :, 0], precision=highest)
        plus = jnp.einsum('srj,sqkpcj->srqkpc', tables[1], packed[:, :, 1:3], precision=highest)
        minus = jnp.einsum('srj,sqkpcj->srqkpc', tables[2], packed[:, :, 1:3], precision=highest)
        plain = plain.reshape(block, RPAIRS, 2, 2, 2, COMPS)
        plus = plus.reshape(block, RPAIRS, 2, 2, 2, 2, COMPS)
        minus = minus.reshape(block, RPAIRS, 2, 2, 2, 2, COMPS)
        return spin_fields(plain, plus, minus)

    blocks = lax.map(one_block, jnp.arange(SLOTS // block, dtype=jnp.int32))
    cycle_sums = blocks.transpose(6, 4, 1, 2, 7, 5, 0, 3).reshape(2 * RPAIRS, 3, 2, COMPS, 2, SLOTS)
    lower_all = slot_orders
    upper_all = L - 1 - lower_all
    coeff = jnp.zeros((2 * RPAIRS, 3, 2, COMPS, L), jnp.float32)
    coeff = coeff.at[..., lower_all].set(cycle_sums[..., 0, :]).at[..., upper_all].set(cycle_sums[..., 1, :])
    shift = jnp.concatenate([cycle_index, cycle_index]) % 2
    orders = jnp.arange(L, dtype=jnp.int32)
    phase = ((orders[None, :] * shift[:, None]) % (2 * NPIX)).astype(jnp.float32) * (math.pi / NPIX)
    factor = jnp.where(orders == 0, 1.0, 2.0).astype(jnp.float32)
    cosine = (jnp.cos(phase) * factor)[:, None, None, :]
    sine = (jnp.sin(phase) * factor)[:, None, None, :]
    real_part = coeff[:, :, 0]
    imag_part = coeff[:, :, 1]
    shifted_real = real_part * cosine - imag_part * sine
    shifted_imag = real_part * sine + imag_part * cosine
    spectrum = shifted_real + 1j * shifted_imag
    padded = jnp.pad(spectrum, ((0, 0), (0, 0), (0, 0), (0, NPIX - L)))
    maps = jnp.real(jnp.fft.ifft(padded, axis=-1)) * NPIX
    return maps.astype(jnp.float32)
```

```python
import functools
import math

import jax
import jax.numpy as jnp
import numpy as np
from jax import lax
from jax.experimental import pallas as pl
from jax.experimental.pallas import tpu as pltpu
from jax.sharding import PartitionSpec as P


def column_weights(lower_order, first_column, columns_count, full_width):
    columns = first_column + jnp.arange(columns_count, dtype=jnp.int32)
    boundary = (full_width - 1 - lower_order)[:, None]
    lower_part = (columns[None, :] < boundary).astype(jnp.float32)
    upper_part = ((columns[None, :] >= boundary) & (columns[None, :] < full_width - 1)).astype(
        jnp.float32
    )
    lower_sign = (1 - 2 * (columns[None, :] % 2)).astype(jnp.float32)
    upper_sign = (1 - 2 * ((columns[None, :] + 1 + lower_order[:, None]) % 2)).astype(jnp.float32)
    return jnp.stack(
        [lower_part, lower_part * lower_sign, upper_part, upper_part * upper_sign], axis=1
    )


def spin_fields(plain, plus, minus):
    hemisphere = jnp.array([1.0, -1.0], jnp.float32).reshape(1, 1, 1, 2, 1, 1, 1)
    minus = minus * hemisphere
    temp_real = plain[:, :, :, :, 0]
    temp_imag = plain[:, :, :, :, 1]
    eplus_real = plus[:, :, :, :, 0, 0]
    eplus_imag = plus[:, :, :, :, 0, 1]
    bplus_real = plus[:, :, :, :, 1, 0]
    bplus_imag = plus[:, :, :, :, 1, 1]
    eminus_real = minus[:, :, :, :, 0, 0]
    eminus_imag = minus[:, :, :, :, 0, 1]
    bminus_real = minus[:, :, :, :, 1, 0]
    bminus_imag = minus[:, :, :, :, 1, 1]
    stokes_q_real = -(eplus_real - bminus_imag)
    stokes_q_imag = -(eplus_imag + bminus_real)
    stokes_u_real = -(bplus_real + eminus_imag)
    stokes_u_imag = -(bplus_imag - eminus_real)
    return jnp.stack(
        [
            jnp.stack([temp_real, temp_imag]),
            jnp.stack([stokes_q_real, stokes_q_imag]),
            jnp.stack([stokes_u_real, stokes_u_imag]),
        ]
    )


def place_orders(cycle_orders, lower_all):
    highest = lax.Precision.HIGHEST
    half = lower_all.shape[0]
    width = min(512, half)
    pieces = []
    for start in range(0, half, width):
        targets = start + jnp.arange(width, dtype=jnp.int32)
        onehot = (lower_all[:, None] == targets[None, :]).astype(jnp.float32)
        pieces.append(jnp.einsum("abcdes,sm->abcdem", cycle_orders, onehot, precision=highest))
    placed = jnp.concatenate(pieces, axis=-1)
    return jnp.concatenate([placed[..., 0, :], jnp.flip(placed[..., 1, :], axis=-1)], axis=-1)


def cycle_synthesis(coeff, shift, first_group, group_count):
    highest = lax.Precision.HIGHEST
    cycles_count = coeff.shape[0]
    components = coeff.shape[3]
    orders_count = coeff.shape[-1]
    pixels = 2 * orders_count
    outer = pixels // 128
    groups = orders_count // 128
    orders = jnp.arange(orders_count, dtype=jnp.int32)
    phase = (orders[None, :] * shift[:, None] % (2 * pixels)).astype(jnp.float32) * (
        math.pi / pixels
    )
    factor = jnp.where(orders == 0, 1.0, 2.0).astype(jnp.float32)
    cosine = (jnp.cos(phase) * factor)[:, None, None, :]
    sine = (jnp.sin(phase) * factor)[:, None, None, :]
    real_part = coeff[:, :, 0]
    imag_part = coeff[:, :, 1]
    shifted_real = (real_part * cosine - imag_part * sine).reshape(
        cycles_count, 3, components, groups, 128
    )
    shifted_imag = (real_part * sine + imag_part * cosine).reshape(
        cycles_count, 3, components, groups, 128
    )
    group_ids = jnp.arange(groups, dtype=jnp.int32)
    outer_ids = jnp.arange(outer, dtype=jnp.int32)
    inner_ids = jnp.arange(128, dtype=jnp.int32)
    angle_one = (group_ids[:, None] * outer_ids[None, :] % outer).astype(jnp.float32) * (
        2.0 * math.pi / outer
    )
    cos_one = jnp.cos(angle_one)
    sin_one = jnp.sin(angle_one)
    first_real = jnp.einsum(
        "xyzab,ak->xyzkb", shifted_real, cos_one, precision=highest
    ) - jnp.einsum("xyzab,ak->xyzkb", shifted_imag, sin_one, precision=highest)
    first_imag = jnp.einsum(
        "xyzab,ak->xyzkb", shifted_real, sin_one, precision=highest
    ) + jnp.einsum("xyzab,ak->xyzkb", shifted_imag, cos_one, precision=highest)
    angle_two = (outer_ids[:, None] * inner_ids[None, :] % pixels).astype(jnp.float32) * (
        2.0 * math.pi / pixels
    )
    cos_two = jnp.cos(angle_two)
    sin_two = jnp.sin(angle_two)
    twist_real = first_real * cos_two - first_imag * sin_two
    twist_imag = first_real * sin_two + first_imag * cos_two
    local_ids = first_group + jnp.arange(group_count, dtype=jnp.int32)
    angle_three = (inner_ids[:, None] * local_ids[None, :] % 128).astype(jnp.float32) * (
        2.0 * math.pi / 128
    )
    cos_three = jnp.cos(angle_three)
    sin_three = jnp.sin(angle_three)
    result = jnp.einsum("xyzkb,bq->xyzqk", twist_real, cos_three, precision=highest) - jnp.einsum(
        "xyzkb,bq->xyzqk", twist_imag, sin_three, precision=highest
    )
    return result.reshape(cycles_count, 3, components, group_count * outer)


def general_body(legendre, harmonics, slot_orders, cycle_index):
    ell_count = lax.axis_size("ell")
    slots_here = harmonics.shape[0]
    columns_here = harmonics.shape[-1]
    components = harmonics.shape[3]
    full_width = 2 * slot_orders.shape[0]
    pairs = cycle_index.shape[0]
    lower_here = lax.dynamic_slice_in_dim(
        slot_orders, lax.axis_index("ma") * slots_here, slots_here
    )
    weights = column_weights(
        lower_here, lax.axis_index("ell") * columns_here, columns_here, full_width
    ).astype(jnp.bfloat16)
    packed = harmonics[:, None] * weights[:, :, None, None, None, :]
    plain = jnp.einsum(
        "srj,sqpcj->srqpc", legendre[0], packed[:, :, 0], preferred_element_type=jnp.float32
    )
    plus = jnp.einsum(
        "srj,sqkpcj->srqkpc", legendre[1], packed[:, :, 1:3], preferred_element_type=jnp.float32
    )
    minus = jnp.einsum(
        "srj,sqkpcj->srqkpc", legendre[2], packed[:, :, 1:3], preferred_element_type=jnp.float32
    )
    plain = plain.reshape(slots_here, pairs, 2, 2, 2, components)
    plus = plus.reshape(slots_here, pairs, 2, 2, 2, 2, components)
    minus = minus.reshape(slots_here, pairs, 2, 2, 2, 2, components)
    fields = spin_fields(plain, plus, minus)
    cycle_sums = fields.transpose(5, 3, 0, 1, 6, 4, 2).reshape(
        2 * pairs, 3, 2, components, 2, slots_here
    )
    summed = lax.psum(cycle_sums, "ell")
    cycle_orders = lax.all_to_all(summed, "ma", split_axis=0, concat_axis=5, tiled=True)
    slot_ids = jnp.arange(slot_orders.shape[0], dtype=jnp.int32)
    lower_all = slot_orders[slot_ids]
    coeff = place_orders(cycle_orders, lower_all)
    cycles_here = cycle_orders.shape[0]
    cycle_ids = lax.axis_index("ma") * cycles_here + jnp.arange(cycles_here, dtype=jnp.int32)
    shift = cycle_index[cycle_ids % pairs] % 2
    per_device = 128 // ell_count
    return cycle_synthesis(coeff, shift, lax.axis_index("ell") * per_device, per_device)


LANES = 128
NT = (((1,), (1,)), ((), ()))
SUB = 32


def rotate_sums(group, lane_pair, sub_pair):
    turned = None
    for step in range(4):
        mixed = group[step]
        for pair in range(1, 4):
            mixed = jnp.where(sub_pair == pair, group[(pair + step) % 4], mixed)
        if step == 0:
            turned = mixed
        else:
            mixed = pltpu.roll(mixed, 2 * step, 0)
            turned = jnp.where((sub_pair - lane_pair) % 4 == step, mixed, turned)
    return turned


def fused_kernel(
    width, slots, columns,
    cycle_hbm, orders_hbm, order_rows_hbm, tables_hbm, packed_hbm,
    phase_hbm, first_hbm, twist_hbm, last_hbm, out_ref,
    cycle_ref, orders_ref, rows_ref, table_ref, even_ref, plain_ref,
    phase_ref, first_ref, twist_ref, last_ref,
    spin_part, plain_part, send_ref, held_ref, left_ref, right_ref, pixel_ref, landed_ref,
    small_sem, spin_sem, plain_sem, send_sem, recv_sem, pixel_send, pixel_recv,
):
    highest = lax.Precision.HIGHEST
    owners, sources = lax.axis_size("ma"), lax.axis_size("ell")
    my_owner, my_source = lax.axis_index("ma"), lax.axis_index("ell")
    me = my_owner * sources + my_source
    mesh_ids = pl.DeviceIdType.MESH
    count = owners * sources
    quads = slots // 4
    half = quads // 2
    subs = quads // SUB
    plain_subs = half // SUB

    small = [
        pltpu.make_async_copy(a, b, small_sem.at[i])
        for i, (a, b) in enumerate(
            [
                (orders_hbm, orders_ref),
                (order_rows_hbm, rows_ref),
                (cycle_hbm, cycle_ref),
                (phase_hbm, phase_ref),
                (first_hbm, first_ref),
                (twist_hbm, twist_ref),
                (last_hbm, last_ref),
            ]
        )
    ]

    def spin_copies(sub):
        here = pl.ds(sub * SUB, SUB)
        copies = []
        for g in range(4):
            copies.append((tables_hbm.at[pl.ds(1, 2), g, here], table_ref.at[pl.ds(1, 2), here, :, g]))
            for k in range(2):
                copies.append((packed_hbm.at[g, here, pl.ds(2, 4), k], even_ref.at[here, k, g]))
        return [
            pltpu.make_async_copy(a, b, spin_sem.at[sub, i]) for i, (a, b) in enumerate(copies)
        ]

    def plain_copies(sub):
        copies = []
        to = pl.ds(sub * SUB, SUB)
        for ab in range(2):
            here = pl.ds(ab * half + sub * SUB, SUB)
            for g in range(4):
                copies.append((tables_hbm.at[0, g, here], table_ref.at[0, here, :, g]))
                for k in range(2):
                    copies.append((packed_hbm.at[g, here, pl.ds(0, 2), k], plain_ref.at[to, k, ab, g]))
        return [
            pltpu.make_async_copy(a, b, plain_sem.at[sub, i]) for i, (a, b) in enumerate(copies)
        ]

    small[0].start()
    small[1].start()

    def start_spin(sub, carry):
        for copy in spin_copies(sub):
            copy.start()
        return carry

    def start_plain(sub, carry):
        for copy in plain_copies(sub):
            copy.start()
        return carry

    lax.fori_loop(0, subs, start_spin, 0)
    lax.fori_loop(0, plain_subs, start_plain, 0)
    for copy in small[2:]:
        copy.start()

    def shifted_device(step):
        owner = lax.rem(my_owner + step // sources, owners)
        source = lax.rem(my_source + step % sources, sources)
        return owner, source

    barrier = pltpu.get_barrier_semaphore()

    def greet(step, carry):
        pl.semaphore_signal(
            barrier, inc=1, device_id=shifted_device(step), device_id_type=mesh_ids
        )
        return carry

    lax.fori_loop(1, count, greet, 0)

    lane8 = lax.broadcasted_iota(jnp.int32, (8, LANES), 1)
    sub8 = lax.broadcasted_iota(jnp.int32, (8, LANES), 0)
    lane_low = lax.broadcasted_iota(jnp.int32, (4, LANES), 1) < 64
    small[0].wait()
    small[1].wait()

    def ordered_rows(owner):
        lower = rows_ref[owner]
        turned = pltpu.roll(lower, 64, 1)
        return jnp.concatenate(
            [
                jnp.where(lane_low, lower, width - 1 - turned),
                jnp.where(lane_low, turned, width - 1 - lower),
            ],
            axis=0,
        )

    lane_rows = lax.broadcasted_iota(jnp.int32, (LANES, LANES), 0)
    for near in range(owners):
        ordered = ordered_rows(lax.rem(my_owner + owners - near, owners))
        for k in range(8):
            at = ((k // 4) * owners + near) * 4 + k % 4
            right_ref[:, at * LANES : (at + 1) * LANES] = jnp.where(
                lane_rows == ordered[k : k + 1, :] % LANES, 1.0, 0.0
            ).astype(jnp.bfloat16)

    first_column = my_source * columns
    lane16 = lax.broadcasted_iota(jnp.int32, (16, LANES), 1)
    sub16 = lax.broadcasted_iota(jnp.int32, (16, LANES), 0)
    alternate = (1 - 2 * (lane16 % 2)).astype(jnp.float32).astype(jnp.bfloat16)
    local = (sub16 // 2 % 2) * LANES + lane16
    inside = jnp.where(first_column + local + 2 * LANES < width - 1, 1.0, 0.0).astype(jnp.bfloat16)
    local8 = (sub8 // 2 % 2) * LANES + lane8
    limit = width - 1 - first_column
    sub_pair = sub8 // 2
    flat_tables = table_ref.reshape(3, quads, 2, 16, LANES)
    flat_even = even_ref.reshape(quads, 2, LANES, LANES)
    flat_plain = plain_ref.reshape(half, 2, LANES, LANES)

    def lower_masks(quad):
        bounds = [limit - orders_ref[my_owner * slots + g * quads + quad] for g in range(4)]
        pairs = [jnp.where(sub8 < 4, bounds[2 * p], bounds[2 * p + 1]) for p in range(2)]
        return [
            jnp.concatenate(
                [jnp.where(local8 + 2 * LANES * k < pair, 1.0, 0.0) for pair in pairs], axis=0
            ).astype(jnp.bfloat16)
            for k in range(2)
        ]

    def weighted(table, quad, masks):
        full = [flat_tables[table, quad, 0], flat_tables[table, quad, 1] * inside]
        low = [full[k] * masks[k] for k in range(2)]
        return [
            jnp.concatenate(pair, axis=1)
            for pair in (full, [v * alternate for v in full], low, [v * alternate for v in low])
        ]

    spin_pair = (lane8 // 32 % 2) * 2 + lane8 // 4 % 2
    plain_pair = (lane8 // 16 % 2) * 2 + lane8 // 4 % 2

    def spin_quad(quad, carry):
        masks = lower_masks(quad)
        left = jnp.concatenate(weighted(1, quad, masks) + weighted(2, quad, masks), axis=0)
        right = jnp.concatenate([flat_even[quad, 0], flat_even[quad, 1]], axis=1)
        product = lax.dot_general(left, right, NT, preferred_element_type=jnp.float32)
        for t in range(2):
            group = []
            for q in range(4):
                at = (t * 4 + q) * 16
                group.append(jnp.where(lane8 < 64, product[at : at + 8], product[at + 8 : at + 16]))
            spin_part[t, pl.ds(pl.multiple_of(quad * 8, 8), 8), :] = rotate_sums(
                group, spin_pair, sub_pair
            )
        return carry

    def plain_octet(octet, carry):
        parts = []
        for ab in range(2):
            quad = octet + ab * half
            parts.append(weighted(0, quad, lower_masks(quad)))
        left = jnp.concatenate([parts[ab][q] for q in range(4) for ab in range(2)], axis=0)
        right = jnp.concatenate([flat_plain[octet, 0], flat_plain[octet, 1]], axis=1)
        product = lax.dot_general(left, right, NT, preferred_element_type=jnp.float32)
        group = []
        for q in range(4):
            chosen = product[q * 32 : q * 32 + 8]
            for g in range(1, 4):
                at = q * 32 + g * 8
                chosen = jnp.where(lane8 // 32 == g, product[at : at + 8], chosen)
            group.append(chosen)
        plain_part[pl.ds(pl.multiple_of(octet * 8, 8), 8), :] = rotate_sums(
            group, plain_pair, sub_pair
        )
        return carry

    def exchange(piece, step):
        owner, source = shifted_device(step)
        return pltpu.make_async_remote_copy(
            src_ref=send_ref.at[piece, owner * sources + source],
            dst_ref=held_ref.at[piece, me],
            send_sem=send_sem.at[piece, step],
            recv_sem=recv_sem.at[piece, step],
            device_id=(owner, source),
            device_id_type=mesh_ids,
        )

    def send_piece(piece):
        def send(step, carry):
            exchange(piece, step).start()
            return carry

        lax.fori_loop(1, count, send, 0)
        held_ref[piece, me] = send_ref[piece, me]

    ordered = ordered_rows(my_owner)
    upper_sign = jnp.where(lane8 < 64, 1.0, (1 - 2 * (ordered % 2)).astype(jnp.float32))
    flat_send = send_ref.reshape(3, count * 8, LANES)

    def by_order(load, south):
        low = load(2 + south)
        return jnp.concatenate([low, load(south) - low], axis=0).T

    def spin_piece(piece, carry):
        def sub_block(sub, inner):
            for copy in spin_copies(sub):
                copy.wait()
            return lax.fori_loop(
                0, SUB, lambda i, c: spin_quad(sub * SUB + i, c), inner, unroll=SUB
            )

        for sub in range(half // SUB):
            sub_block(piece * (half // SUB) + sub, 0)
        first = piece * half * 8
        sign = jnp.where(piece == 0, upper_sign[0:4], upper_sign[4:8])
        for south in range(2):
            for r in range(2):
                plus, minus = (
                    by_order(lambda q: spin_part[t, pl.ds(first + q * 2 + r, half, stride=8), :], south)
                    for t in range(2)
                )
                if south:
                    minus = -minus
                for g in range(4):
                    at = g * 32
                    ep_re, ep_im, bp_re, bp_im = (plus[at + 8 * i : at + 8 * i + 8] for i in range(4))
                    em_re, em_im, bm_re, bm_im = (minus[at + 8 * i : at + 8 * i + 8] for i in range(4))
                    values = (bm_im - ep_re, -(ep_im + bm_re), -(bp_re + em_im), em_re - bp_im)
                    for i, value in enumerate(values):
                        value = value + pltpu.roll(value, 4, 0)
                        if south:
                            value = value * sign[g : g + 1, :]
                        row = ((south * 2 + r) * sources + (i // 2) * 4) * 8 + (i % 2) * 4 + g
                        flat_send[piece, pl.ds(row, 4, stride=8), :] = value[0:4]

        @pl.when(piece == 0)
        def _():
            pl.semaphore_wait(barrier, count - 1)

        send_piece(piece)
        return carry

    lax.fori_loop(0, 2, spin_piece, 0)

    def plain_block(sub, carry):
        for copy in plain_copies(sub):
            copy.wait()
        return lax.fori_loop(
            0, SUB, lambda i, c: plain_octet(sub * SUB + i, c), carry, unroll=SUB
        )

    lax.fori_loop(0, plain_subs, plain_block, 0)
    for south in range(2):
        for r in range(2):
            turned = by_order(lambda q: plain_part[pl.ds(q * 2 + r, half, stride=8), :], south)
            for k in range(8):
                real, imag = turned[k * 16 : k * 16 + 8], turned[k * 16 + 8 : k * 16 + 16]
                value = jnp.where(
                    sub8 < 4, real + pltpu.roll(real, 4, 0), imag + pltpu.roll(imag, 4, 0)
                )
                if south:
                    value = value * upper_sign[k : k + 1, :]
                row = (south * 2 + r) * sources * 8 + k
                flat_send[2, pl.ds(row, 8, stride=8), :] = value
    send_piece(2)
    for copy in small[2:]:
        copy.wait()

    tall = width // LANES
    tall_ids = lax.broadcasted_iota(jnp.int32, (tall, LANES), 0)

    def received(piece, near):
        def await_step(step, carry):
            exchange(piece, step).wait()
            return carry

        lax.fori_loop(max(1, near * sources), (near + 1) * sources, await_step, 0)
        owner = lax.rem(my_owner + owners - near, owners)
        total = held_ref[piece, owner * sources]
        for source in range(1, sources):
            total = total + held_ref[piece, owner * sources + source]
        high = total.astype(jnp.bfloat16).astype(jnp.float32)
        rest = total - high
        middle = rest.astype(jnp.bfloat16).astype(jnp.float32)
        return ordered_rows(owner), (high, middle, rest - middle)

    def place(ordered_row, pieces, row, left_row, at):
        here = tall_ids == ordered_row // LANES
        for i in range(3):
            to = left_row + i * tall
            left_ref[to : to + tall, at * LANES : (at + 1) * LANES] = jnp.where(
                here, pieces[i][row : row + 1, :], 0.0
            ).astype(jnp.bfloat16)

    def place_spin(piece):
        for near in range(owners):
            ordered, pieces = received(piece, near)
            for g in range(4):
                at = (piece * owners + near) * 4 + g
                for part in range(2):
                    place(
                        ordered[piece * 4 + g : piece * 4 + g + 1, :],
                        pieces, part * 4 + g, part * 3 * tall, at,
                    )
        span = pl.ds(piece * owners * 4 * LANES, owners * 4 * LANES)
        return lax.dot_general(
            left_ref[0 : 6 * tall, span], right_ref[:, span], NT, preferred_element_type=jnp.float32
        )

    def joined(placed, at):
        return placed[at : at + tall] + placed[at + tall : at + 2 * tall] + placed[at + 2 * tall : at + 3 * tall]

    wide = 2 * tall

    def pixel_copy(which, step):
        source = lax.rem(my_source + step, sources)
        return pltpu.make_async_remote_copy(
            src_ref=pixel_ref.at[which, source],
            dst_ref=landed_ref.at[which, my_source],
            send_sem=pixel_send.at[which, step],
            recv_sem=pixel_recv.at[which, step],
            device_id=(my_owner, source),
            device_id_type=mesh_ids,
        )

    def transform(which, real_part, imag_part):
        spectrum = jnp.concatenate([real_part, imag_part], axis=0)
        first = jnp.dot(
            first_ref[...], spectrum, precision=highest, preferred_element_type=jnp.float32
        )
        real, imag = first[:wide], first[wide:]
        twisted = jnp.concatenate(
            [
                real * twist_ref[0] - imag * twist_ref[1],
                real * twist_ref[1] + imag * twist_ref[0],
            ],
            axis=1,
        )
        both = lax.dot_general(
            last_ref[...], twisted, NT, precision=highest, preferred_element_type=jnp.float32
        )
        pixels = jnp.concatenate([both[:wide], both[wide:]], axis=1)
        for e in range(sources):
            pixel_ref[which, e] = pixels[e * 8 : e * 8 + 8]
        for step in range(1, sources):
            pixel_copy(which, step).start()
        landed_ref[which, my_source] = pixel_ref[which, my_source]

    shifted = cycle_ref[lax.rem(my_owner, cycle_ref.shape[0])] % 2 == 1
    factor = phase_ref[2]
    cosine = jnp.where(shifted, phase_ref[0], factor)
    sine = jnp.where(shifted, phase_ref[1], 0.0)

    placed = place_spin(0)
    placed = placed + place_spin(1)
    real, imag = joined(placed, 0), joined(placed, 3 * tall)
    transform(0, real * cosine - imag * sine, real * sine + imag * cosine)

    for near in range(owners):
        ordered, pieces = received(2, near)
        for k in range(8):
            at = ((k // 4) * owners + near) * 4 + k % 4
            place(ordered[k : k + 1, :], pieces, k, 0, at)
    placed = lax.dot_general(
        left_ref[0 : 3 * tall, :], right_ref[...], NT, preferred_element_type=jnp.float32
    )
    value = joined(placed, 0)
    is_real = my_source < sources // 2
    transform(1, value * jnp.where(is_real, cosine, -sine), value * jnp.where(is_real, sine, cosine))
    for which in range(2):
        for step in range(1, sources):
            pixel_copy(which, step).wait()
    for c in range(4):
        out_ref[c] = landed_ref[1, c] + landed_ref[1, 4 + c]
        out_ref[4 + c] = landed_ref[0, c]
        out_ref[8 + c] = landed_ref[0, 4 + c]


def synthesis_tables(orders_count):
    pixels = 2 * orders_count
    tall = orders_count // LANES
    half = 2 * tall
    orders = np.arange(orders_count).reshape(tall, LANES)
    factor = np.where(orders == 0, 1.0, 2.0)
    angle = orders * (np.pi / pixels)
    phase = np.stack([np.cos(angle) * factor, np.sin(angle) * factor, factor])
    angle = (np.arange(half)[:, None] * np.arange(tall)[None, :] % half) * (2 * np.pi / half)
    first = np.block([[np.cos(angle), -np.sin(angle)], [np.sin(angle), np.cos(angle)]])
    angle = np.arange(half)[:, None] * np.arange(LANES)[None, :] * (2 * np.pi / pixels)
    twist = np.stack([np.cos(angle), np.sin(angle)])
    ids = np.concatenate([np.arange(0, LANES, 2), np.arange(1, LANES, 2)])
    angle = (ids[:, None] * np.arange(LANES)[None, :] % LANES) * (2 * np.pi / LANES)
    last = np.concatenate([np.cos(angle), -np.sin(angle)], axis=1)
    return [jnp.asarray(t, jnp.float32) for t in (phase, first, twist, last)]


def packed_body(legendre, harmonics, slot_orders, cycle_index):
    owners, sources = lax.axis_size("ma"), lax.axis_size("ell")
    slots, columns = harmonics.shape[0], harmonics.shape[-1]
    width = 2 * slot_orders.shape[0]
    quads, tall, count = slots // 4, width // LANES, owners * sources
    tables = (
        legendre.reshape(3, slots, 2, 4, LANES)
        .transpose(0, 1, 3, 2, 4)
        .reshape(3, 4, quads, 2, 4, LANES)
    )
    packed = (
        harmonics.reshape(slots, 3, 2, 4, 4, LANES)
        .transpose(0, 1, 2, 4, 3, 5)
        .reshape(4, quads, 6, 2, 8, LANES)
    )
    constants = synthesis_tables(width)
    anywhere = pl.BlockSpec(memory_space=pl.ANY)
    dma = pltpu.SemaphoreType.DMA
    maps = pl.pallas_call(
        functools.partial(fused_kernel, width, slots, columns),
        in_specs=[anywhere] * 9,
        out_specs=pl.BlockSpec(memory_space=pltpu.VMEM),
        out_shape=jax.ShapeDtypeStruct((12, 8, LANES), jnp.float32),
        scratch_shapes=[
            pltpu.SMEM(cycle_index.shape, jnp.int32),
            pltpu.SMEM(slot_orders.shape, jnp.int32),
            pltpu.VMEM((owners, 4, LANES), jnp.int32),
            pltpu.VMEM((3, quads, 2, 4, 4, LANES), jnp.bfloat16),
            pltpu.VMEM((quads, 2, 4, 4, 8, LANES), jnp.bfloat16),
            pltpu.VMEM((quads // 2, 2, 2, 4, 2, 8, LANES), jnp.bfloat16),
            *(pltpu.VMEM(c.shape, c.dtype) for c in constants),
            pltpu.VMEM((2, quads * 8, LANES), jnp.float32),
            pltpu.VMEM((quads * 4, LANES), jnp.float32),
            pltpu.VMEM((3, count, 8, LANES), jnp.float32),
            pltpu.VMEM((3, count, 8, LANES), jnp.float32),
            pltpu.VMEM((6 * tall, width), jnp.bfloat16),
            pltpu.VMEM((LANES, width), jnp.bfloat16),
            pltpu.VMEM((2, sources, 8, LANES), jnp.float32),
            pltpu.VMEM((2, sources, 8, LANES), jnp.float32),
            dma((7,)),
            dma((quads // SUB, 12)),
            dma((quads // 2 // SUB, 24)),
            dma((3, count)),
            dma((3, count)),
            dma((2, sources)),
            dma((2, sources)),
        ],
        compiler_params=pltpu.CompilerParams(
            vmem_limit_bytes=60 * 1024 * 1024, collective_id=0, has_side_effects=True
        ),
    )(cycle_index, slot_orders, slot_orders.reshape(owners, 4, LANES), tables, packed, *constants)
    return maps.reshape(1, 3, 4, 8 * LANES)


def body(legendre, harmonics, slot_orders, cycle_index):
    owners, sources = lax.axis_size("ma"), lax.axis_size("ell")
    slots, kinds, parts, components, columns = harmonics.shape
    pairs = cycle_index.shape[0]
    fits = (
        (pairs, components, columns, slots) == (2, 4, 4 * LANES, 4 * LANES)
        and owners == 2 * pairs
        and kinds * parts * components == 3 * sources
        and slot_orders.shape[0] * 4 == sources * 8 * LANES
    )
    chosen = packed_body if fits else general_body
    return chosen(legendre, harmonics, slot_orders, cycle_index)


def solution(mesh):
    return jax.shard_map(
        body,
        mesh=mesh,
        in_specs=(P(None, "ma", None, "ell"), P("ma", None, None, None, "ell"), P(), P()),
        out_specs=P("ma", None, None, "ell"),
        check_vma=False,
    )
```

```python
import functools
import math

import jax
import jax.numpy as jnp
import numpy as np
from jax import lax
from jax.experimental import pallas as pl
from jax.experimental.pallas import tpu as pltpu
from jax.sharding import PartitionSpec as P


def column_weights(lower_order, first_column, columns_count, full_width):
    columns = first_column + jnp.arange(columns_count, dtype=jnp.int32)
    boundary = (full_width - 1 - lower_order)[:, None]
    lower_part = (columns[None, :] < boundary).astype(jnp.float32)
    upper_part = ((columns[None, :] >= boundary) & (columns[None, :] < full_width - 1)).astype(
        jnp.float32
    )
    lower_sign = (1 - 2 * (columns[None, :] % 2)).astype(jnp.float32)
    upper_sign = (1 - 2 * ((columns[None, :] + 1 + lower_order[:, None]) % 2)).astype(jnp.float32)
    return jnp.stack(
        [lower_part, lower_part * lower_sign, upper_part, upper_part * upper_sign], axis=1
    )


def spin_fields(plain, plus, minus):
    hemisphere = jnp.array([1.0, -1.0], jnp.float32).reshape(1, 1, 1, 2, 1, 1, 1)
    minus = minus * hemisphere
    temp_real = plain[:, :, :, :, 0]
    temp_imag = plain[:, :, :, :, 1]
    eplus_real = plus[:, :, :, :, 0, 0]
    eplus_imag = plus[:, :, :, :, 0, 1]
    bplus_real = plus[:, :, :, :, 1, 0]
    bplus_imag = plus[:, :, :, :, 1, 1]
    eminus_real = minus[:, :, :, :, 0, 0]
    eminus_imag = minus[:, :, :, :, 0, 1]
    bminus_real = minus[:, :, :, :, 1, 0]
    bminus_imag = minus[:, :, :, :, 1, 1]
    stokes_q_real = -(eplus_real - bminus_imag)
    stokes_q_imag = -(eplus_imag + bminus_real)
    stokes_u_real = -(bplus_real + eminus_imag)
    stokes_u_imag = -(bplus_imag - eminus_real)
    return jnp.stack(
        [
            jnp.stack([temp_real, temp_imag]),
            jnp.stack([stokes_q_real, stokes_q_imag]),
            jnp.stack([stokes_u_real, stokes_u_imag]),
        ]
    )


def place_orders(cycle_orders, lower_all):
    highest = lax.Precision.HIGHEST
    half = lower_all.shape[0]
    width = min(512, half)
    pieces = []
    for start in range(0, half, width):
        targets = start + jnp.arange(width, dtype=jnp.int32)
        onehot = (lower_all[:, None] == targets[None, :]).astype(jnp.float32)
        pieces.append(jnp.einsum("abcdes,sm->abcdem", cycle_orders, onehot, precision=highest))
    placed = jnp.concatenate(pieces, axis=-1)
    return jnp.concatenate([placed[..., 0, :], jnp.flip(placed[..., 1, :], axis=-1)], axis=-1)


def cycle_synthesis(coeff, shift, first_group, group_count):
    highest = lax.Precision.HIGHEST
    cycles_count = coeff.shape[0]
    components = coeff.shape[3]
    orders_count = coeff.shape[-1]
    pixels = 2 * orders_count
    outer = pixels // 128
    groups = orders_count // 128
    orders = jnp.arange(orders_count, dtype=jnp.int32)
    phase = (orders[None, :] * shift[:, None] % (2 * pixels)).astype(jnp.float32) * (
        math.pi / pixels
    )
    factor = jnp.where(orders == 0, 1.0, 2.0).astype(jnp.float32)
    cosine = (jnp.cos(phase) * factor)[:, None, None, :]
    sine = (jnp.sin(phase) * factor)[:, None, None, :]
    real_part = coeff[:, :, 0]
    imag_part = coeff[:, :, 1]
    shifted_real = (real_part * cosine - imag_part * sine).reshape(
        cycles_count, 3, components, groups, 128
    )
    shifted_imag = (real_part * sine + imag_part * cosine).reshape(
        cycles_count, 3, components, groups, 128
    )
    group_ids = jnp.arange(groups, dtype=jnp.int32)
    outer_ids = jnp.arange(outer, dtype=jnp.int32)
    inner_ids = jnp.arange(128, dtype=jnp.int32)
    angle_one = (group_ids[:, None] * outer_ids[None, :] % outer).astype(jnp.float32) * (
        2.0 * math.pi / outer
    )
    cos_one = jnp.cos(angle_one)
    sin_one = jnp.sin(angle_one)
    first_real = jnp.einsum(
        "xyzab,ak->xyzkb", shifted_real, cos_one, precision=highest
    ) - jnp.einsum("xyzab,ak->xyzkb", shifted_imag, sin_one, precision=highest)
    first_imag = jnp.einsum(
        "xyzab,ak->xyzkb", shifted_real, sin_one, precision=highest
    ) + jnp.einsum("xyzab,ak->xyzkb", shifted_imag, cos_one, precision=highest)
    angle_two = (outer_ids[:, None] * inner_ids[None, :] % pixels).astype(jnp.float32) * (
        2.0 * math.pi / pixels
    )
    cos_two = jnp.cos(angle_two)
    sin_two = jnp.sin(angle_two)
    twist_real = first_real * cos_two - first_imag * sin_two
    twist_imag = first_real * sin_two + first_imag * cos_two
    local_ids = first_group + jnp.arange(group_count, dtype=jnp.int32)
    angle_three = (inner_ids[:, None] * local_ids[None, :] % 128).astype(jnp.float32) * (
        2.0 * math.pi / 128
    )
    cos_three = jnp.cos(angle_three)
    sin_three = jnp.sin(angle_three)
    result = jnp.einsum("xyzkb,bq->xyzqk", twist_real, cos_three, precision=highest) - jnp.einsum(
        "xyzkb,bq->xyzqk", twist_imag, sin_three, precision=highest
    )
    return result.reshape(cycles_count, 3, components, group_count * outer)


def general_body(legendre, harmonics, slot_orders, cycle_index):
    ell_count = lax.axis_size("ell")
    slots_here = harmonics.shape[0]
    columns_here = harmonics.shape[-1]
    components = harmonics.shape[3]
    full_width = 2 * slot_orders.shape[0]
    pairs = cycle_index.shape[0]
    lower_here = lax.dynamic_slice_in_dim(
        slot_orders, lax.axis_index("ma") * slots_here, slots_here
    )
    weights = column_weights(
        lower_here, lax.axis_index("ell") * columns_here, columns_here, full_width
    ).astype(jnp.bfloat16)
    packed = harmonics[:, None] * weights[:, :, None, None, None, :]
    plain = jnp.einsum(
        "srj,sqpcj->srqpc", legendre[0], packed[:, :, 0], preferred_element_type=jnp.float32
    )
    plus = jnp.einsum(
        "srj,sqkpcj->srqkpc", legendre[1], packed[:, :, 1:3], preferred_element_type=jnp.float32
    )
    minus = jnp.einsum(
        "srj,sqkpcj->srqkpc", legendre[2], packed[:, :, 1:3], preferred_element_type=jnp.float32
    )
    plain = plain.reshape(slots_here, pairs, 2, 2, 2, components)
    plus = plus.reshape(slots_here, pairs, 2, 2, 2, 2, components)
    minus = minus.reshape(slots_here, pairs, 2, 2, 2, 2, components)
    fields = spin_fields(plain, plus, minus)
    cycle_sums = fields.transpose(5, 3, 0, 1, 6, 4, 2).reshape(
        2 * pairs, 3, 2, components, 2, slots_here
    )
    summed = lax.psum(cycle_sums, "ell")
    cycle_orders = lax.all_to_all(summed, "ma", split_axis=0, concat_axis=5, tiled=True)
    slot_ids = jnp.arange(slot_orders.shape[0], dtype=jnp.int32)
    lower_all = slot_orders[slot_ids]
    coeff = place_orders(cycle_orders, lower_all)
    cycles_here = cycle_orders.shape[0]
    cycle_ids = lax.axis_index("ma") * cycles_here + jnp.arange(cycles_here, dtype=jnp.int32)
    shift = cycle_index[cycle_ids % pairs] % 2
    per_device = 128 // ell_count
    return cycle_synthesis(coeff, shift, lax.axis_index("ell") * per_device, per_device)


LANES = 128
NT = (((1,), (1,)), ((), ()))
SUB = 32


def rotate_sums(group, lane_pair, sub_pair):
    turned = None
    for step in range(4):
        mixed = group[step]
        for pair in range(1, 4):
            mixed = jnp.where(sub_pair == pair, group[(pair + step) % 4], mixed)
        if step == 0:
            turned = mixed
        else:
            mixed = pltpu.roll(mixed, 2 * step, 0)
            turned = jnp.where((sub_pair - lane_pair) % 4 == step, mixed, turned)
    return turned


def fused_kernel(
    width, slots, columns,
    cycle_hbm, orders_hbm, order_rows_hbm, tables_hbm, packed_hbm,
    phase_hbm, first_hbm, twist_hbm, last_hbm, out_ref,
    cycle_ref, orders_ref, rows_ref, table_ref, even_ref, plain_ref,
    phase_ref, first_ref, twist_ref, last_ref,
    spin_part, plain_part, send_ref, fold_ref, half_ref, held_ref, left_ref, right_ref, pixel_ref, landed_ref,
    small_sem, spin_sem, plain_sem, fold_send, fold_recv, send_sem, recv_sem, pixel_send, pixel_recv,
):
    highest = lax.Precision.HIGHEST
    owners, sources = lax.axis_size("ma"), lax.axis_size("ell")
    my_owner, my_source = lax.axis_index("ma"), lax.axis_index("ell")
    mesh_ids = pl.DeviceIdType.MESH
    quads = slots // 4
    half = quads // 2
    subs = quads // SUB
    plain_subs = half // SUB

    small = [
        pltpu.make_async_copy(a, b, small_sem.at[i])
        for i, (a, b) in enumerate(
            [
                (orders_hbm, orders_ref),
                (order_rows_hbm, rows_ref),
                (cycle_hbm, cycle_ref),
                (phase_hbm, phase_ref),
                (first_hbm, first_ref),
                (twist_hbm, twist_ref),
                (last_hbm, last_ref),
            ]
        )
    ]

    def spin_copies(sub):
        here = pl.ds(sub * SUB, SUB)
        copies = []
        for g in range(4):
            copies.append((tables_hbm.at[pl.ds(1, 2), g, here], table_ref.at[pl.ds(1, 2), here, :, g]))
            for k in range(2):
                copies.append((packed_hbm.at[g, here, pl.ds(2, 4), k], even_ref.at[here, k, g]))
        return [
            pltpu.make_async_copy(a, b, spin_sem.at[sub, i]) for i, (a, b) in enumerate(copies)
        ]

    def plain_copies(sub):
        copies = []
        to = pl.ds(sub * SUB, SUB)
        for ab in range(2):
            here = pl.ds(ab * half + sub * SUB, SUB)
            for g in range(4):
                copies.append((tables_hbm.at[0, g, here], table_ref.at[0, here, :, g]))
                for k in range(2):
                    copies.append((packed_hbm.at[g, here, pl.ds(0, 2), k], plain_ref.at[to, k, ab, g]))
        return [
            pltpu.make_async_copy(a, b, plain_sem.at[sub, i]) for i, (a, b) in enumerate(copies)
        ]

    small[0].start()
    small[1].start()

    def start_spin(sub, carry):
        for copy in spin_copies(sub):
            copy.start()
        return carry

    def start_plain(sub, carry):
        for copy in plain_copies(sub):
            copy.start()
        return carry

    lax.fori_loop(0, subs, start_spin, 0)
    lax.fori_loop(0, plain_subs, start_plain, 0)
    for copy in small[2:]:
        copy.start()

    def wrapped(place, step, size):
        place = place + step
        return jnp.where(place >= size, place - size, place)

    lines = sources // 2
    my_line, my_side = my_source // 2, my_source % 2
    near_owner = [wrapped(my_owner, i, owners) for i in range(owners)]
    near_line = [wrapped(my_line, i, lines) for i in range(lines)]
    spread = owners * lines

    def shifted_device(step):
        return near_owner[step // lines], near_line[step % lines] * 2 + my_side

    barrier = pltpu.get_barrier_semaphore()

    met = [shifted_device(step) for step in range(1, spread)]
    met += [(my_owner, near_line[i] * 2 + 1 - my_side) for i in range(lines)]
    for device in reversed(met):
        pl.semaphore_signal(barrier, inc=1, device_id=device, device_id_type=mesh_ids)

    lane8 = lax.broadcasted_iota(jnp.int32, (8, LANES), 1)
    sub8 = lax.broadcasted_iota(jnp.int32, (8, LANES), 0)
    lane_low = lax.broadcasted_iota(jnp.int32, (4, LANES), 1) < 64
    small[0].wait()
    small[1].wait()

    def ordered_rows(owner):
        lower = rows_ref[owner]
        turned = pltpu.roll(lower, 64, 1)
        return jnp.concatenate(
            [
                jnp.where(lane_low, lower, width - 1 - turned),
                jnp.where(lane_low, turned, width - 1 - lower),
            ],
            axis=0,
        )

    first_column = my_source * columns
    lane16 = lax.broadcasted_iota(jnp.int32, (16, LANES), 1)
    sub16 = lax.broadcasted_iota(jnp.int32, (16, LANES), 0)
    alternate = (1 - 2 * (lane16 % 2)).astype(jnp.float32).astype(jnp.bfloat16)
    local = (sub16 // 2 % 2) * LANES + lane16
    inside = jnp.where(first_column + local + 2 * LANES < width - 1, 1.0, 0.0).astype(jnp.bfloat16)
    local8 = (sub8 // 2 % 2) * LANES + lane8
    limit = width - 1 - first_column
    sub_pair = sub8 // 2
    flat_even = even_ref.reshape(quads, 2, LANES, LANES)
    flat_plain = plain_ref.reshape(half, 2, LANES, LANES)

    def lower_masks(quad):
        bounds = [limit - orders_ref[my_owner * slots + g * quads + quad] for g in range(4)]
        pairs = [jnp.where(sub8 < 4, bounds[2 * p], bounds[2 * p + 1]) for p in range(2)]
        return [
            jnp.concatenate(
                [jnp.where(local8 + 2 * LANES * k < pair, 1.0, 0.0) for pair in pairs], axis=0
            ).astype(jnp.bfloat16)
            for k in range(2)
        ]

    def weighted(table, quad, masks):
        full = [
            jnp.concatenate([table_ref[table, quad, k, g] for g in range(4)], axis=0)
            for k in range(2)
        ]
        full[1] = full[1] * inside
        low = [full[k] * masks[k] for k in range(2)]
        return [
            jnp.concatenate(pair, axis=1)
            for pair in (full, [v * alternate for v in full], low, [v * alternate for v in low])
        ]

    spin_pair = (lane8 // 32 % 2) * 2 + lane8 // 4 % 2
    plain_pair = (lane8 // 16 % 2) * 2 + lane8 // 4 % 2

    def spin_quad(quad, carry):
        masks = lower_masks(quad)
        left = jnp.concatenate(weighted(1, quad, masks) + weighted(2, quad, masks), axis=0)
        right = jnp.concatenate([flat_even[quad, 0], flat_even[quad, 1]], axis=1)
        product = lax.dot_general(left, right, NT, preferred_element_type=jnp.float32)
        for t in range(2):
            group = []
            for q in range(4):
                at = (t * 4 + q) * 16
                group.append(jnp.where(lane8 < 64, product[at : at + 8], product[at + 8 : at + 16]))
            spin_part[t, pl.ds(pl.multiple_of(quad * 8, 8), 8), :] = rotate_sums(
                group, spin_pair, sub_pair
            )
        return carry

    def plain_octet(octet, carry):
        parts = []
        for ab in range(2):
            quad = octet + ab * half
            parts.append(weighted(0, quad, lower_masks(quad)))
        left = jnp.concatenate([parts[ab][q] for q in range(4) for ab in range(2)], axis=0)
        right = jnp.concatenate([flat_plain[octet, 0], flat_plain[octet, 1]], axis=1)
        product = lax.dot_general(left, right, NT, preferred_element_type=jnp.float32)
        group = []
        for q in range(4):
            chosen = product[q * 32 : q * 32 + 8]
            for g in range(1, 4):
                at = q * 32 + g * 8
                chosen = jnp.where(lane8 // 32 == g, product[at : at + 8], chosen)
            group.append(chosen)
        plain_part[pl.ds(pl.multiple_of(octet * 8, 8), 8), :] = rotate_sums(
            group, plain_pair, sub_pair
        )
        return carry

    def fold(piece):
        return pltpu.make_async_remote_copy(
            src_ref=send_ref.at[piece, :, 1 - my_side],
            dst_ref=fold_ref.at[piece],
            send_sem=fold_send.at[piece],
            recv_sem=fold_recv.at[piece],
            device_id=(my_owner, my_line * 2 + 1 - my_side),
            device_id_type=mesh_ids,
        )

    def exchange(piece, step):
        owner, line = near_owner[step // lines], near_line[step % lines]
        return pltpu.make_async_remote_copy(
            src_ref=half_ref.at[piece, owner, line],
            dst_ref=held_ref.at[piece, my_owner, my_line],
            send_sem=send_sem.at[piece, step],
            recv_sem=recv_sem.at[piece, step],
            device_id=(owner, line * 2 + my_side),
            device_id_type=mesh_ids,
        )

    def forward_piece(piece):
        fold(piece).wait_recv()
        for owner in range(owners):
            for line in range(lines):
                half_ref[piece, owner, line] = (
                    send_ref[piece, owner, my_side, line] + fold_ref[piece, owner, line]
                )
        for step in range(1, spread):
            exchange(piece, step).start()
        held_ref[piece, my_owner, my_line] = half_ref[piece, my_owner, my_line]

    ordered = ordered_rows(my_owner)
    upper_sign = jnp.where(lane8 < 64, 1.0, (1 - 2 * (ordered % 2)).astype(jnp.float32))
    flat_send = send_ref.reshape(3, owners * sources * 8, LANES)

    def by_order(load, south):
        low = load(2 + south)
        return jnp.concatenate([low, load(south) - low], axis=0).T

    def finish_spin(piece):
        first = piece * half * 8
        sign = jnp.where(piece == 0, upper_sign[0:4], upper_sign[4:8])
        for south in range(2):
            for r in range(2):
                plus, minus = (
                    by_order(lambda q: spin_part[t, pl.ds(first + q * 2 + r, half, stride=8), :], south)
                    for t in range(2)
                )
                if south:
                    minus = -minus
                for g in range(4):
                    at = g * 32
                    ep_re, ep_im, bp_re, bp_im = (plus[at + 8 * i : at + 8 * i + 8] for i in range(4))
                    em_re, em_im, bm_re, bm_im = (minus[at + 8 * i : at + 8 * i + 8] for i in range(4))
                    values = (bm_im - ep_re, -(ep_im + bm_re), -(bp_re + em_im), em_re - bp_im)
                    for i, value in enumerate(values):
                        value = value + pltpu.roll(value, 4, 0)
                        if south:
                            value = value * sign[g : g + 1, :]
                        row = ((south * 2 + r) * sources + (i // 2) * 4) * 8 + (i % 2) * 4 + g
                        flat_send[piece, pl.ds(row, 4, stride=8), :] = value[0:4]

    per_piece = half // SUB

    def spin_block(sub, carry):
        for copy in spin_copies(sub):
            copy.wait()
        lax.fori_loop(0, SUB, lambda i, c: spin_quad(sub * SUB + i, c), 0, unroll=SUB)

        @pl.when(lax.rem(sub, per_piece) == per_piece - 1)
        def _():
            finish_spin(lax.div(sub, per_piece))

        @pl.when(sub == per_piece)
        def _():
            pl.semaphore_wait(barrier, len(met))
            fold(0).start()

        return carry

    lax.fori_loop(0, subs, spin_block, 0)
    fold(1).start()

    def plain_block(sub, carry):
        @pl.when(sub == plain_subs - 1)
        def _():
            forward_piece(0)

        for copy in plain_copies(sub):
            copy.wait()
        return lax.fori_loop(
            0, SUB, lambda i, c: plain_octet(sub * SUB + i, c), carry, unroll=SUB
        )

    lax.fori_loop(0, plain_subs, plain_block, 0)
    for south in range(2):
        for r in range(2):
            turned = by_order(lambda q: plain_part[pl.ds(q * 2 + r, half, stride=8), :], south)
            for k in range(8):
                real, imag = turned[k * 16 : k * 16 + 8], turned[k * 16 + 8 : k * 16 + 16]
                value = jnp.where(
                    sub8 < 4, real + pltpu.roll(real, 4, 0), imag + pltpu.roll(imag, 4, 0)
                )
                if south:
                    value = value * upper_sign[k : k + 1, :]
                row = (south * 2 + r) * sources * 8 + k
                flat_send[2, pl.ds(row, 8, stride=8), :] = value
    fold(2).start()
    forward_piece(1)
    lane_rows = lax.broadcasted_iota(jnp.int32, (LANES, LANES), 0)
    for near in range(owners):
        ordered = ordered_rows(lax.rem(my_owner + owners - near, owners))
        for k in range(8):
            at = ((k // 4) * owners + near) * 4 + k % 4
            right_ref[:, at * LANES : (at + 1) * LANES] = jnp.where(
                lane_rows == ordered[k : k + 1, :] % LANES, 1.0, 0.0
            ).astype(jnp.bfloat16)
    for copy in small[2:]:
        copy.wait()
    forward_piece(2)

    tall = width // LANES
    tall_ids = lax.broadcasted_iota(jnp.int32, (tall, LANES), 0)

    def received(piece, near):
        for step in range(max(1, near * lines), (near + 1) * lines):
            exchange(piece, step).wait()
        owner = lax.rem(my_owner + owners - near, owners)
        total = held_ref[piece, owner, 0]
        for line in range(1, lines):
            total = total + held_ref[piece, owner, line]
        high = total.astype(jnp.bfloat16).astype(jnp.float32)
        rest = total - high
        middle = rest.astype(jnp.bfloat16).astype(jnp.float32)
        return ordered_rows(owner), (high, middle, rest - middle)

    def place(ordered_row, pieces, row, left_row, at):
        here = tall_ids == ordered_row // LANES
        for i in range(3):
            to = left_row + i * tall
            left_ref[to : to + tall, at * LANES : (at + 1) * LANES] = jnp.where(
                here, pieces[i][row : row + 1, :], 0.0
            ).astype(jnp.bfloat16)

    def place_spin(piece):
        for near in range(owners):
            ordered, pieces = received(piece, near)
            for g in range(4):
                at = (piece * owners + near) * 4 + g
                for part in range(2):
                    place(
                        ordered[piece * 4 + g : piece * 4 + g + 1, :],
                        pieces, part * 4 + g, part * 3 * tall, at,
                    )
        span = pl.ds(piece * owners * 4 * LANES, owners * 4 * LANES)
        return lax.dot_general(
            left_ref[0 : 6 * tall, span], right_ref[:, span], NT, preferred_element_type=jnp.float32
        )

    def joined(placed, at):
        return placed[at : at + tall] + placed[at + tall : at + 2 * tall] + placed[at + 2 * tall : at + 3 * tall]

    wide = 2 * tall

    def pixel_copy(which, step):
        source = lax.rem(my_source + step, sources)
        return pltpu.make_async_remote_copy(
            src_ref=pixel_ref.at[which, source],
            dst_ref=landed_ref.at[which, my_source],
            send_sem=pixel_send.at[which, step],
            recv_sem=pixel_recv.at[which, step],
            device_id=(my_owner, source),
            device_id_type=mesh_ids,
        )

    def transform(which, real_part, imag_part):
        spectrum = jnp.concatenate([real_part, imag_part], axis=0)
        first = jnp.dot(
            first_ref[...], spectrum, precision=highest, preferred_element_type=jnp.float32
        )
        real, imag = first[:wide], first[wide:]
        twisted = jnp.concatenate(
            [
                real * twist_ref[0] - imag * twist_ref[1],
                real * twist_ref[1] + imag * twist_ref[0],
            ],
            axis=1,
        )
        both = lax.dot_general(
            last_ref[...], twisted, NT, precision=highest, preferred_element_type=jnp.float32
        )
        pixels = jnp.concatenate([both[:wide], both[wide:]], axis=1)
        for e in range(sources):
            pixel_ref[which, e] = pixels[e * 8 : e * 8 + 8]
        for step in range(1, sources):
            pixel_copy(which, step).start()
        landed_ref[which, my_source] = pixel_ref[which, my_source]

    shifted = cycle_ref[lax.rem(my_owner, cycle_ref.shape[0])] % 2 == 1
    factor = phase_ref[2]
    cosine = jnp.where(shifted, phase_ref[0], factor)
    sine = jnp.where(shifted, phase_ref[1], 0.0)

    placed = place_spin(0)
    placed = placed + place_spin(1)
    real, imag = joined(placed, 0), joined(placed, 3 * tall)
    transform(0, real * cosine - imag * sine, real * sine + imag * cosine)

    for near in range(owners):
        ordered, pieces = received(2, near)
        for k in range(8):
            at = ((k // 4) * owners + near) * 4 + k % 4
            place(ordered[k : k + 1, :], pieces, k, 0, at)
    placed = lax.dot_general(
        left_ref[0 : 3 * tall, :], right_ref[...], NT, preferred_element_type=jnp.float32
    )
    value = joined(placed, 0)
    is_real = my_side == 0
    transform(1, value * jnp.where(is_real, cosine, -sine), value * jnp.where(is_real, sine, cosine))
    for piece in range(3):
        fold(piece).wait_send()
    for which in range(2):
        for step in range(1, sources):
            pixel_copy(which, step).wait()
    for c in range(4):
        out_ref[c] = landed_ref[1, 2 * c] + landed_ref[1, 2 * c + 1]
        out_ref[4 + c] = landed_ref[0, 2 * c]
        out_ref[8 + c] = landed_ref[0, 2 * c + 1]


def synthesis_tables(orders_count):
    pixels = 2 * orders_count
    tall = orders_count // LANES
    half = 2 * tall
    orders = np.arange(orders_count).reshape(tall, LANES)
    factor = np.where(orders == 0, 1.0, 2.0)
    angle = orders * (np.pi / pixels)
    phase = np.stack([np.cos(angle) * factor, np.sin(angle) * factor, factor])
    angle = (np.arange(half)[:, None] * np.arange(tall)[None, :] % half) * (2 * np.pi / half)
    first = np.block([[np.cos(angle), -np.sin(angle)], [np.sin(angle), np.cos(angle)]])
    angle = np.arange(half)[:, None] * np.arange(LANES)[None, :] * (2 * np.pi / pixels)
    twist = np.stack([np.cos(angle), np.sin(angle)])
    ids = np.concatenate([np.arange(0, LANES, 2), np.arange(1, LANES, 2)])
    angle = (ids[:, None] * np.arange(LANES)[None, :] % LANES) * (2 * np.pi / LANES)
    last = np.concatenate([np.cos(angle), -np.sin(angle)], axis=1)
    return [jnp.asarray(t, jnp.float32) for t in (phase, first, twist, last)]


def packed_body(legendre, harmonics, slot_orders, cycle_index):
    owners, sources = lax.axis_size("ma"), lax.axis_size("ell")
    slots, columns = harmonics.shape[0], harmonics.shape[-1]
    width = 2 * slot_orders.shape[0]
    quads, tall, lines = slots // 4, width // LANES, sources // 2
    tables = (
        legendre.reshape(3, slots, 2, 4, LANES)
        .transpose(0, 1, 3, 2, 4)
        .reshape(3, 4, quads, 2, 4, LANES)
    )
    packed = (
        harmonics.reshape(slots, 3, 2, 4, 4, LANES)
        .transpose(0, 1, 2, 4, 3, 5)
        .reshape(4, quads, 6, 2, 8, LANES)
    )
    constants = synthesis_tables(width)
    operands = [
        pltpu.with_memory_space_constraint(x, pltpu.HBM)
        for x in (
            cycle_index, slot_orders, slot_orders.reshape(owners, 4, LANES), tables, packed, *constants
        )
    ]
    anywhere = pl.BlockSpec(memory_space=pl.ANY)
    dma = pltpu.SemaphoreType.DMA
    maps = pl.pallas_call(
        functools.partial(fused_kernel, width, slots, columns),
        in_specs=[anywhere] * 9,
        out_specs=pl.BlockSpec(memory_space=pltpu.VMEM),
        out_shape=jax.ShapeDtypeStruct((12, 8, LANES), jnp.float32),
        scratch_shapes=[
            pltpu.SMEM(cycle_index.shape, jnp.int32),
            pltpu.SMEM(slot_orders.shape, jnp.int32),
            pltpu.VMEM((owners, 4, LANES), jnp.int32),
            pltpu.VMEM((3, quads, 2, 4, 4, LANES), jnp.bfloat16),
            pltpu.VMEM((quads, 2, 4, 4, 8, LANES), jnp.bfloat16),
            pltpu.VMEM((quads // 2, 2, 2, 4, 2, 8, LANES), jnp.bfloat16),
            *(pltpu.VMEM(c.shape, c.dtype) for c in constants),
            pltpu.VMEM((2, quads * 8, LANES), jnp.float32),
            pltpu.VMEM((quads * 4, LANES), jnp.float32),
            pltpu.VMEM((3, owners, 2, lines, 8, LANES), jnp.float32),
            pltpu.VMEM((3, owners, lines, 8, LANES), jnp.float32),
            pltpu.VMEM((3, owners, lines, 8, LANES), jnp.float32),
            pltpu.VMEM((3, owners, lines, 8, LANES), jnp.float32),
            pltpu.VMEM((6 * tall, width), jnp.bfloat16),
            pltpu.VMEM((LANES, width), jnp.bfloat16),
            pltpu.VMEM((2, sources, 8, LANES), jnp.float32),
            pltpu.VMEM((2, sources, 8, LANES), jnp.float32),
            dma((7,)),
            dma((quads // SUB, 12)),
            dma((quads // 2 // SUB, 24)),
            dma((3,)),
            dma((3,)),
            dma((3, owners * lines)),
            dma((3, owners * lines)),
            dma((2, sources)),
            dma((2, sources)),
        ],
        compiler_params=pltpu.CompilerParams(
            vmem_limit_bytes=40 * 1024 * 1024, collective_id=0, has_side_effects=True
        ),
    )(*operands)
    return maps.reshape(1, 3, 4, 8 * LANES)


def body(legendre, harmonics, slot_orders, cycle_index):
    owners, sources = lax.axis_size("ma"), lax.axis_size("ell")
    slots, kinds, parts, components, columns = harmonics.shape
    pairs = cycle_index.shape[0]
    fits = (
        (pairs, components, columns, slots) == (2, 4, 4 * LANES, 4 * LANES)
        and owners == 2 * pairs
        and kinds * parts * components == 3 * sources
        and slot_orders.shape[0] * 4 == sources * 8 * LANES
    )
    chosen = packed_body if fits else general_body
    return chosen(legendre, harmonics, slot_orders, cycle_index)


def solution(mesh):
    return jax.shard_map(
        body,
        mesh=mesh,
        in_specs=(P(None, "ma", None, "ell"), P("ma", None, None, None, "ell"), P(), P()),
        out_specs=P("ma", None, None, "ell"),
        check_vma=False,
    )
```

```python
import functools
import math

import jax
import jax.numpy as jnp
import numpy as np
from jax import lax
from jax.experimental import pallas as pl
from jax.experimental.pallas import tpu as pltpu
from jax.sharding import PartitionSpec as P


def column_weights(lower_order, first_column, columns_count, full_width):
    columns = first_column + jnp.arange(columns_count, dtype=jnp.int32)
    boundary = (full_width - 1 - lower_order)[:, None]
    lower_part = (columns[None, :] < boundary).astype(jnp.float32)
    upper_part = ((columns[None, :] >= boundary) & (columns[None, :] < full_width - 1)).astype(
        jnp.float32
    )
    lower_sign = (1 - 2 * (columns[None, :] % 2)).astype(jnp.float32)
    upper_sign = (1 - 2 * ((columns[None, :] + 1 + lower_order[:, None]) % 2)).astype(jnp.float32)
    return jnp.stack(
        [lower_part, lower_part * lower_sign, upper_part, upper_part * upper_sign], axis=1
    )


def spin_fields(plain, plus, minus):
    hemisphere = jnp.array([1.0, -1.0], jnp.float32).reshape(1, 1, 1, 2, 1, 1, 1)
    minus = minus * hemisphere
    temp_real = plain[:, :, :, :, 0]
    temp_imag = plain[:, :, :, :, 1]
    eplus_real = plus[:, :, :, :, 0, 0]
    eplus_imag = plus[:, :, :, :, 0, 1]
    bplus_real = plus[:, :, :, :, 1, 0]
    bplus_imag = plus[:, :, :, :, 1, 1]
    eminus_real = minus[:, :, :, :, 0, 0]
    eminus_imag = minus[:, :, :, :, 0, 1]
    bminus_real = minus[:, :, :, :, 1, 0]
    bminus_imag = minus[:, :, :, :, 1, 1]
    stokes_q_real = -(eplus_real - bminus_imag)
    stokes_q_imag = -(eplus_imag + bminus_real)
    stokes_u_real = -(bplus_real + eminus_imag)
    stokes_u_imag = -(bplus_imag - eminus_real)
    return jnp.stack(
        [
            jnp.stack([temp_real, temp_imag]),
            jnp.stack([stokes_q_real, stokes_q_imag]),
            jnp.stack([stokes_u_real, stokes_u_imag]),
        ]
    )


def place_orders(cycle_orders, lower_all):
    highest = lax.Precision.HIGHEST
    half = lower_all.shape[0]
    width = min(512, half)
    pieces = []
    for start in range(0, half, width):
        targets = start + jnp.arange(width, dtype=jnp.int32)
        onehot = (lower_all[:, None] == targets[None, :]).astype(jnp.float32)
        pieces.append(jnp.einsum("abcdes,sm->abcdem", cycle_orders, onehot, precision=highest))
    placed = jnp.concatenate(pieces, axis=-1)
    return jnp.concatenate([placed[..., 0, :], jnp.flip(placed[..., 1, :], axis=-1)], axis=-1)


def cycle_synthesis(coeff, shift, first_group, group_count):
    highest = lax.Precision.HIGHEST
    cycles_count = coeff.shape[0]
    components = coeff.shape[3]
    orders_count = coeff.shape[-1]
    pixels = 2 * orders_count
    outer = pixels // 128
    groups = orders_count // 128
    orders = jnp.arange(orders_count, dtype=jnp.int32)
    phase = (orders[None, :] * shift[:, None] % (2 * pixels)).astype(jnp.float32) * (
        math.pi / pixels
    )
    factor = jnp.where(orders == 0, 1.0, 2.0).astype(jnp.float32)
    cosine = (jnp.cos(phase) * factor)[:, None, None, :]
    sine = (jnp.sin(phase) * factor)[:, None, None, :]
    real_part = coeff[:, :, 0]
    imag_part = coeff[:, :, 1]
    shifted_real = (real_part * cosine - imag_part * sine).reshape(
        cycles_count, 3, components, groups, 128
    )
    shifted_imag = (real_part * sine + imag_part * cosine).reshape(
        cycles_count, 3, components, groups, 128
    )
    group_ids = jnp.arange(groups, dtype=jnp.int32)
    outer_ids = jnp.arange(outer, dtype=jnp.int32)
    inner_ids = jnp.arange(128, dtype=jnp.int32)
    angle_one = (group_ids[:, None] * outer_ids[None, :] % outer).astype(jnp.float32) * (
        2.0 * math.pi / outer
    )
    cos_one = jnp.cos(angle_one)
    sin_one = jnp.sin(angle_one)
    first_real = jnp.einsum(
        "xyzab,ak->xyzkb", shifted_real, cos_one, precision=highest
    ) - jnp.einsum("xyzab,ak->xyzkb", shifted_imag, sin_one, precision=highest)
    first_imag = jnp.einsum(
        "xyzab,ak->xyzkb", shifted_real, sin_one, precision=highest
    ) + jnp.einsum("xyzab,ak->xyzkb", shifted_imag, cos_one, precision=highest)
    angle_two = (outer_ids[:, None] * inner_ids[None, :] % pixels).astype(jnp.float32) * (
        2.0 * math.pi / pixels
    )
    cos_two = jnp.cos(angle_two)
    sin_two = jnp.sin(angle_two)
    twist_real = first_real * cos_two - first_imag * sin_two
    twist_imag = first_real * sin_two + first_imag * cos_two
    local_ids = first_group + jnp.arange(group_count, dtype=jnp.int32)
    angle_three = (inner_ids[:, None] * local_ids[None, :] % 128).astype(jnp.float32) * (
        2.0 * math.pi / 128
    )
    cos_three = jnp.cos(angle_three)
    sin_three = jnp.sin(angle_three)
    result = jnp.einsum("xyzkb,bq->xyzqk", twist_real, cos_three, precision=highest) - jnp.einsum(
        "xyzkb,bq->xyzqk", twist_imag, sin_three, precision=highest
    )
    return result.reshape(cycles_count, 3, components, group_count * outer)


def general_body(legendre, harmonics, slot_orders, cycle_index):
    ell_count = lax.axis_size("ell")
    slots_here = harmonics.shape[0]
    columns_here = harmonics.shape[-1]
    components = harmonics.shape[3]
    full_width = 2 * slot_orders.shape[0]
    pairs = cycle_index.shape[0]
    lower_here = lax.dynamic_slice_in_dim(
        slot_orders, lax.axis_index("ma") * slots_here, slots_here
    )
    weights = column_weights(
        lower_here, lax.axis_index("ell") * columns_here, columns_here, full_width
    ).astype(jnp.bfloat16)
    packed = harmonics[:, None] * weights[:, :, None, None, None, :]
    plain = jnp.einsum(
        "srj,sqpcj->srqpc", legendre[0], packed[:, :, 0], preferred_element_type=jnp.float32
    )
    plus = jnp.einsum(
        "srj,sqkpcj->srqkpc", legendre[1], packed[:, :, 1:3], preferred_element_type=jnp.float32
    )
    minus = jnp.einsum(
        "srj,sqkpcj->srqkpc", legendre[2], packed[:, :, 1:3], preferred_element_type=jnp.float32
    )
    plain = plain.reshape(slots_here, pairs, 2, 2, 2, components)
    plus = plus.reshape(slots_here, pairs, 2, 2, 2, 2, components)
    minus = minus.reshape(slots_here, pairs, 2, 2, 2, 2, components)
    fields = spin_fields(plain, plus, minus)
    cycle_sums = fields.transpose(5, 3, 0, 1, 6, 4, 2).reshape(
        2 * pairs, 3, 2, components, 2, slots_here
    )
    summed = lax.psum(cycle_sums, "ell")
    cycle_orders = lax.all_to_all(summed, "ma", split_axis=0, concat_axis=5, tiled=True)
    slot_ids = jnp.arange(slot_orders.shape[0], dtype=jnp.int32)
    lower_all = slot_orders[slot_ids]
    coeff = place_orders(cycle_orders, lower_all)
    cycles_here = cycle_orders.shape[0]
    cycle_ids = lax.axis_index("ma") * cycles_here + jnp.arange(cycles_here, dtype=jnp.int32)
    shift = cycle_index[cycle_ids % pairs] % 2
    per_device = 128 // ell_count
    return cycle_synthesis(coeff, shift, lax.axis_index("ell") * per_device, per_device)


LANES = 128
NT = (((1,), (1,)), ((), ()))
SUB = 32


def rotate_sums(group, lane_pair, sub_pair):
    turned = None
    for step in range(4):
        mixed = group[step]
        for pair in range(1, 4):
            mixed = jnp.where(sub_pair == pair, group[(pair + step) % 4], mixed)
        if step == 0:
            turned = mixed
        else:
            mixed = pltpu.roll(mixed, 2 * step, 0)
            turned = jnp.where((sub_pair - lane_pair) % 4 == step, mixed, turned)
    return turned


def fused_kernel(
    width, slots, columns,
    cycle_hbm, orders_hbm, order_rows_hbm, tables_hbm, packed_hbm,
    phase_hbm, first_hbm, twist_hbm, last_hbm, out_ref,
    cycle_ref, orders_ref, rows_ref, table_ref, even_ref, plain_ref,
    phase_ref, first_ref, twist_ref, last_ref,
    spin_part, plain_part, send_ref, held_ref, left_ref, right_ref, pixel_ref, landed_ref,
    small_sem, spin_sem, plain_sem, send_sem, recv_sem, pixel_send, pixel_recv,
):
    owners, sources = lax.axis_size("ma"), lax.axis_size("ell")
    my_owner, my_source = lax.axis_index("ma"), lax.axis_index("ell")
    mesh_ids = pl.DeviceIdType.MESH
    quads = slots // 4
    half = quads // 2
    subs = quads // SUB
    plain_subs = half // SUB

    small = [
        pltpu.make_async_copy(a, b, small_sem.at[i])
        for i, (a, b) in enumerate(
            [
                (orders_hbm, orders_ref),
                (order_rows_hbm, rows_ref),
                (cycle_hbm, cycle_ref),
                (phase_hbm, phase_ref),
                (first_hbm, first_ref),
                (twist_hbm, twist_ref),
                (last_hbm, last_ref),
            ]
        )
    ]

    def spin_copies(sub):
        here = pl.ds(sub * SUB, SUB)
        copies = []
        for g in range(4):
            copies.append((tables_hbm.at[pl.ds(1, 2), g, here], table_ref.at[pl.ds(1, 2), here, :, g]))
            for k in range(2):
                copies.append((packed_hbm.at[g, here, pl.ds(2, 4), k], even_ref.at[here, k, g]))
        return [
            pltpu.make_async_copy(a, b, spin_sem.at[sub, i]) for i, (a, b) in enumerate(copies)
        ]

    def plain_copies(sub):
        copies = []
        to = pl.ds(sub * SUB, SUB)
        for ab in range(2):
            here = pl.ds(ab * half + sub * SUB, SUB)
            for g in range(4):
                copies.append((tables_hbm.at[0, g, here], table_ref.at[0, here, :, g]))
                for k in range(2):
                    copies.append((packed_hbm.at[g, here, pl.ds(0, 2), k], plain_ref.at[to, k, ab, g]))
        return [
            pltpu.make_async_copy(a, b, plain_sem.at[sub, i]) for i, (a, b) in enumerate(copies)
        ]

    def wrapped(place, step, size):
        place = place + step
        return jnp.where(place >= size, place - size, place)

    lines = sources // 2
    my_line, my_side = my_source // 2, my_source % 2
    near_owner = [wrapped(my_owner, i, owners) for i in range(owners)]
    near_line = [wrapped(my_line, i, lines) for i in range(lines)]
    rising = my_line * 2 >= lines
    far_line = [
        wrapped(my_line, jnp.where(rising, i, lines - i), lines) for i in range(1, lines)
    ]
    far_line.append(my_line)
    far_owner = [near_owner[i] for i in (*range(1, owners), 0)]
    others = [
        (owner, line, side)
        for i, line in enumerate(far_line)
        for side in (1 - my_side, my_side)
        for j, owner in enumerate(far_owner)
        if (i, side is my_side, j) != (lines - 1, True, owners - 1)
    ]
    same_owner = [d for d in others if d[0] is near_owner[0]]

    barrier = pltpu.get_barrier_semaphore()

    for owner, line, side in others:
        pl.semaphore_signal(
            barrier, inc=1, device_id=(owner, line * 2 + side), device_id_type=mesh_ids
        )

    small[0].start()
    small[1].start()

    def start_spin(sub, carry):
        for copy in spin_copies(sub):
            copy.start()
        return carry

    def start_plain(sub, carry):
        for copy in plain_copies(sub):
            copy.start()
        return carry

    lax.fori_loop(0, subs, start_spin, 0)
    lax.fori_loop(0, plain_subs, start_plain, 0)
    for copy in small[2:]:
        copy.start()

    lane8 = lax.broadcasted_iota(jnp.int32, (8, LANES), 1)
    sub8 = lax.broadcasted_iota(jnp.int32, (8, LANES), 0)
    lane_low = lax.broadcasted_iota(jnp.int32, (4, LANES), 1) < 64
    small[0].wait()
    small[1].wait()

    def ordered_rows(owner):
        lower = rows_ref[owner]
        turned = pltpu.roll(lower, 64, 1)
        return jnp.concatenate(
            [
                jnp.where(lane_low, lower, width - 1 - turned),
                jnp.where(lane_low, turned, width - 1 - lower),
            ],
            axis=0,
        )

    first_column = my_source * columns
    lane16 = lax.broadcasted_iota(jnp.int32, (16, LANES), 1)
    sub16 = lax.broadcasted_iota(jnp.int32, (16, LANES), 0)
    alternate = (1 - 2 * (lane16 % 2)).astype(jnp.float32).astype(jnp.bfloat16)
    local = (sub16 // 2 % 2) * LANES + lane16
    inside = jnp.where(first_column + local + 2 * LANES < width - 1, 1.0, 0.0).astype(jnp.bfloat16)
    local8 = (sub8 // 2 % 2) * LANES + lane8
    limit = width - 1 - first_column
    sub_pair = sub8 // 2
    flat_even = even_ref.reshape(quads, 2, LANES, LANES)
    flat_plain = plain_ref.reshape(half, 2, LANES, LANES)

    def lower_masks(quad):
        bounds = [limit - orders_ref[my_owner * slots + g * quads + quad] for g in range(4)]
        pairs = [jnp.where(sub8 < 4, bounds[2 * p], bounds[2 * p + 1]) for p in range(2)]
        return [
            jnp.concatenate(
                [jnp.where(local8 + 2 * LANES * k < pair, 1.0, 0.0) for pair in pairs], axis=0
            ).astype(jnp.bfloat16)
            for k in range(2)
        ]

    def weighted(table, quad, masks):
        full = [
            jnp.concatenate([table_ref[table, quad, k, g] for g in range(4)], axis=0)
            for k in range(2)
        ]
        full[1] = full[1] * inside
        low = [full[k] * masks[k] for k in range(2)]
        return [
            jnp.concatenate(pair, axis=1)
            for pair in (full, [v * alternate for v in full], low, [v * alternate for v in low])
        ]

    spin_pair = (lane8 // 32 % 2) * 2 + lane8 // 4 % 2
    plain_pair = (lane8 // 16 % 2) * 2 + lane8 // 4 % 2

    def spin_quad(quad, carry):
        masks = lower_masks(quad)
        left = jnp.concatenate(weighted(1, quad, masks) + weighted(2, quad, masks), axis=0)
        right = jnp.concatenate([flat_even[quad, 0], flat_even[quad, 1]], axis=1)
        product = lax.dot_general(left, right, NT, preferred_element_type=jnp.float32)
        for t in range(2):
            group = []
            for q in range(4):
                at = (t * 4 + q) * 16
                group.append(jnp.where(lane8 < 64, product[at : at + 8], product[at + 8 : at + 16]))
            spin_part[t, pl.ds(pl.multiple_of(quad * 8, 8), 8), :] = rotate_sums(
                group, spin_pair, sub_pair
            )
        return carry

    def plain_octet(octet, carry):
        parts = []
        for ab in range(2):
            quad = octet + ab * half
            parts.append(weighted(0, quad, lower_masks(quad)))
        left = jnp.concatenate([parts[ab][q] for q in range(4) for ab in range(2)], axis=0)
        right = jnp.concatenate([flat_plain[octet, 0], flat_plain[octet, 1]], axis=1)
        product = lax.dot_general(left, right, NT, preferred_element_type=jnp.float32)
        group = []
        for q in range(4):
            chosen = product[q * 32 : q * 32 + 8]
            for g in range(1, 4):
                at = q * 32 + g * 8
                chosen = jnp.where(lane8 // 32 == g, product[at : at + 8], chosen)
            group.append(chosen)
        plain_part[pl.ds(pl.multiple_of(octet * 8, 8), 8), :] = rotate_sums(
            group, plain_pair, sub_pair
        )
        return carry

    def exchange(piece, to, origin):
        owner, line, side = to
        return pltpu.make_async_remote_copy(
            src_ref=send_ref.at[piece, owner, side, line],
            dst_ref=held_ref.at[piece, my_owner, my_side, my_line],
            send_sem=send_sem.at[piece, owner, side, line],
            recv_sem=recv_sem.at[(piece, *origin)],
            device_id=(owner, line * 2 + side),
            device_id_type=mesh_ids,
        )

    def send_piece(piece):
        for device in others:
            exchange(piece, device, (my_owner, my_side, my_line)).start()
        held_ref[piece, my_owner, my_side, my_line] = send_ref[piece, my_owner, my_side, my_line]

    ordered = ordered_rows(my_owner)
    upper_sign = jnp.where(lane8 < 64, 1.0, (1 - 2 * (ordered % 2)).astype(jnp.float32))
    flat_send = send_ref.reshape(3, owners * sources * 8, LANES)

    def by_order(load, south):
        low = load(2 + south)
        return jnp.concatenate([low, load(south) - low], axis=0).T

    def finish_spin(piece):
        first = piece * half * 8
        sign = jnp.where(piece == 0, upper_sign[0:4], upper_sign[4:8])
        for south in range(2):
            for r in range(2):
                plus, minus = (
                    by_order(lambda q: spin_part[t, pl.ds(first + q * 2 + r, half, stride=8), :], south)
                    for t in range(2)
                )
                if south:
                    minus = -minus
                for g in range(4):
                    at = g * 32
                    ep_re, ep_im, bp_re, bp_im = (plus[at + 8 * i : at + 8 * i + 8] for i in range(4))
                    em_re, em_im, bm_re, bm_im = (minus[at + 8 * i : at + 8 * i + 8] for i in range(4))
                    values = (bm_im - ep_re, -(ep_im + bm_re), -(bp_re + em_im), em_re - bp_im)
                    for i, value in enumerate(values):
                        value = value + pltpu.roll(value, 4, 0)
                        if south:
                            value = value * sign[g : g + 1, :]
                        row = ((south * 2 + r) * sources + (i // 2) * 4) * 8 + (i % 2) * 4 + g
                        flat_send[piece, pl.ds(row, 4, stride=8), :] = value[0:4]

    per_piece = half // SUB

    def spin_block(sub, carry):
        for copy in spin_copies(sub):
            copy.wait()
        lax.fori_loop(0, SUB, lambda i, c: spin_quad(sub * SUB + i, c), 0, unroll=SUB)

        @pl.when(lax.rem(sub, per_piece) == per_piece - 1)
        def _():
            finish_spin(lax.div(sub, per_piece))

        @pl.when(sub == per_piece - 1)
        def _():
            pl.semaphore_wait(barrier, len(others))
            send_piece(0)

        return carry

    lax.fori_loop(0, subs, spin_block, 0)
    send_piece(1)

    def plain_block(sub, carry):
        for copy in plain_copies(sub):
            copy.wait()
        return lax.fori_loop(
            0, SUB, lambda i, c: plain_octet(sub * SUB + i, c), carry, unroll=SUB
        )

    lax.fori_loop(0, plain_subs, plain_block, 0)
    for south in range(2):
        for r in range(2):
            turned = by_order(lambda q: plain_part[pl.ds(q * 2 + r, half, stride=8), :], south)
            for k in range(8):
                real, imag = turned[k * 16 : k * 16 + 8], turned[k * 16 + 8 : k * 16 + 16]
                value = jnp.where(
                    sub8 < 4, real + pltpu.roll(real, 4, 0), imag + pltpu.roll(imag, 4, 0)
                )
                if south:
                    value = value * upper_sign[k : k + 1, :]
                row = (south * 2 + r) * sources * 8 + k
                flat_send[2, pl.ds(row, 8, stride=8), :] = value
    send_piece(2)
    lane_rows = lax.broadcasted_iota(jnp.int32, (LANES, LANES), 0)
    for near in range(owners):
        ordered = ordered_rows(lax.rem(my_owner + owners - near, owners))
        for k in range(8):
            at = ((k // 4) * owners + near) * 4 + k % 4
            right_ref[:, at * LANES : (at + 1) * LANES] = jnp.where(
                lane_rows == ordered[k : k + 1, :] % LANES, 1.0, 0.0
            ).astype(jnp.bfloat16)
    for copy in small[2:]:
        copy.wait()

    tall = width // LANES
    tall_ids = lax.broadcasted_iota(jnp.int32, (tall, LANES), 0)

    def split(total):
        high = total.astype(jnp.bfloat16).astype(jnp.float32)
        return high, total - high

    def received(piece, near):
        owner = near_owner[-near % owners]
        for i in range(lines):
            for side in (my_side, 1 - my_side):
                if near or i or side is not my_side:
                    device = (owner, near_line[i], side)
                    exchange(piece, device, (owner, side, near_line[i])).wait_recv()
        total = held_ref[piece, owner, 0, 0] + held_ref[piece, owner, 1, 0]
        for line in range(1, lines):
            total = total + held_ref[piece, owner, 0, line] + held_ref[piece, owner, 1, line]
        return ordered_rows(owner), split(total)

    def place(ordered_row, pieces, row, left_row, at):
        here = tall_ids == ordered_row // LANES
        for i in range(2):
            to = left_row + i * tall
            left_ref[to : to + tall, at * LANES : (at + 1) * LANES] = jnp.where(
                here, pieces[i][row : row + 1, :], 0.0
            ).astype(jnp.bfloat16)

    def place_spin(piece):
        for near in range(owners):
            ordered, pieces = received(piece, near)
            for g in range(4):
                at = (piece * owners + near) * 4 + g
                for part in range(2):
                    place(
                        ordered[piece * 4 + g : piece * 4 + g + 1, :],
                        pieces, part * 4 + g, part * 2 * tall, at,
                    )
        span = pl.ds(piece * owners * 4 * LANES, owners * 4 * LANES)
        return lax.dot_general(
            left_ref[0 : 4 * tall, span], right_ref[:, span], NT, preferred_element_type=jnp.float32
        )

    def joined(placed, at):
        return placed[at : at + tall] + placed[at + tall : at + 2 * tall]

    wide = 2 * tall

    def pixel_copy(which, to, origin):
        source = to[1] * 2 + to[2]
        return pltpu.make_async_remote_copy(
            src_ref=pixel_ref.at[which, source],
            dst_ref=landed_ref.at[which, my_source],
            send_sem=pixel_send.at[which, source],
            recv_sem=pixel_recv.at[which, origin],
            device_id=(my_owner, source),
            device_id_type=mesh_ids,
        )

    def halves(value, axis):
        high = value.astype(jnp.bfloat16)
        low = (value - high.astype(jnp.float32)).astype(jnp.bfloat16)
        return jnp.concatenate([high, low, high], axis=axis)

    def transform(which, real_part, imag_part):
        spectrum = halves(jnp.concatenate([real_part, imag_part], axis=0), 0)
        first = jnp.dot(first_ref[...], spectrum, preferred_element_type=jnp.float32)
        real, imag = first[:wide], first[wide:]
        twisted = jnp.concatenate(
            [
                real * twist_ref[0] - imag * twist_ref[1],
                real * twist_ref[1] + imag * twist_ref[0],
            ],
            axis=1,
        )
        both = lax.dot_general(
            last_ref[...], halves(twisted, 1), NT, preferred_element_type=jnp.float32
        )
        pixels = jnp.concatenate([both[:wide], both[wide:]], axis=1)
        for e in range(sources):
            pixel_ref[which, e] = pixels[e * 8 : e * 8 + 8]
        for device in same_owner:
            pixel_copy(which, device, my_source).start()
        landed_ref[which, my_source] = pixel_ref[which, my_source]

    shifted = cycle_ref[lax.rem(my_owner, cycle_ref.shape[0])] % 2 == 1
    factor = phase_ref[2]
    cosine = jnp.where(shifted, phase_ref[0], factor)
    sine = jnp.where(shifted, phase_ref[1], 0.0)

    placed = place_spin(0)
    placed = placed + place_spin(1)
    real, imag = joined(placed, 0), joined(placed, 2 * tall)
    transform(0, real * cosine - imag * sine, real * sine + imag * cosine)

    placed = None
    for near in range(owners):
        ordered, pieces = received(2, near)
        for k in range(8):
            at = ((k // 4) * owners + near) * 4 + k % 4
            place(ordered[k : k + 1, :], pieces, k, 0, at)
        for ab in range(2):
            span = pl.ds((ab * owners + near) * 4 * LANES, 4 * LANES)
            term = lax.dot_general(
                left_ref[0 : 2 * tall, span], right_ref[:, span], NT, preferred_element_type=jnp.float32
            )
            placed = term if placed is None else placed + term
    value = joined(placed, 0)
    is_real = my_side == 0
    transform(1, value * jnp.where(is_real, cosine, -sine), value * jnp.where(is_real, sine, cosine))
    for piece in range(3):
        for owner, line, side in others:
            exchange(piece, (owner, line, side), (owner, side, line)).wait_send()
    for which in range(2):
        for device in same_owner:
            pixel_copy(which, device, device[1] * 2 + device[2]).wait()
    for c in range(4):
        out_ref[c] = landed_ref[1, 2 * c] + landed_ref[1, 2 * c + 1]
        out_ref[4 + c] = landed_ref[0, 2 * c]
        out_ref[8 + c] = landed_ref[0, 2 * c + 1]


def synthesis_tables(orders_count):
    pixels = 2 * orders_count
    tall = orders_count // LANES
    half = 2 * tall
    orders = np.arange(orders_count).reshape(tall, LANES)
    factor = np.where(orders == 0, 1.0, 2.0)
    angle = orders * (np.pi / pixels)
    phase = np.stack([np.cos(angle) * factor, np.sin(angle) * factor, factor])
    angle = (np.arange(half)[:, None] * np.arange(tall)[None, :] % half) * (2 * np.pi / half)
    first = np.block([[np.cos(angle), -np.sin(angle)], [np.sin(angle), np.cos(angle)]])
    angle = np.arange(half)[:, None] * np.arange(LANES)[None, :] * (2 * np.pi / pixels)
    twist = np.stack([np.cos(angle), np.sin(angle)])
    ids = np.concatenate([np.arange(0, LANES, 2), np.arange(1, LANES, 2)])
    angle = (ids[:, None] * np.arange(LANES)[None, :] % LANES) * (2 * np.pi / LANES)
    last = np.concatenate([np.cos(angle), -np.sin(angle)], axis=1)

    def halved(table):
        high = table.astype(jnp.bfloat16)
        low = (table - high.astype(np.float64)).astype(jnp.bfloat16)
        return jnp.asarray(np.concatenate([high, high, low], axis=1))

    return [
        jnp.asarray(phase, jnp.float32), halved(first), jnp.asarray(twist, jnp.float32), halved(last)
    ]


def packed_body(legendre, harmonics, slot_orders, cycle_index):
    owners, sources = lax.axis_size("ma"), lax.axis_size("ell")
    slots, columns = harmonics.shape[0], harmonics.shape[-1]
    width = 2 * slot_orders.shape[0]
    quads, tall, lines = slots // 4, width // LANES, sources // 2
    tables = (
        legendre.reshape(3, slots, 2, 4, LANES)
        .transpose(0, 1, 3, 2, 4)
        .reshape(3, 4, quads, 2, 4, LANES)
    )
    packed = (
        harmonics.reshape(slots, 3, 2, 4, 4, LANES)
        .transpose(0, 1, 2, 4, 3, 5)
        .reshape(4, quads, 6, 2, 8, LANES)
    )
    constants = synthesis_tables(width)
    operands = [
        pltpu.with_memory_space_constraint(x, pltpu.HBM)
        for x in (
            cycle_index, slot_orders, slot_orders.reshape(owners, 4, LANES), tables, packed, *constants
        )
    ]
    anywhere = pl.BlockSpec(memory_space=pl.ANY)
    dma = pltpu.SemaphoreType.DMA
    maps = pl.pallas_call(
        functools.partial(fused_kernel, width, slots, columns),
        in_specs=[anywhere] * 9,
        out_specs=pl.BlockSpec(memory_space=pltpu.VMEM),
        out_shape=jax.ShapeDtypeStruct((12, 8, LANES), jnp.float32),
        scratch_shapes=[
            pltpu.SMEM(cycle_index.shape, jnp.int32),
            pltpu.SMEM(slot_orders.shape, jnp.int32),
            pltpu.VMEM((owners, 4, LANES), jnp.int32),
            pltpu.VMEM((3, quads, 2, 4, 4, LANES), jnp.bfloat16),
            pltpu.VMEM((quads, 2, 4, 4, 8, LANES), jnp.bfloat16),
            pltpu.VMEM((quads // 2, 2, 2, 4, 2, 8, LANES), jnp.bfloat16),
            *(pltpu.VMEM(c.shape, c.dtype) for c in constants),
            pltpu.VMEM((2, quads * 8, LANES), jnp.float32),
            pltpu.VMEM((quads * 4, LANES), jnp.float32),
            pltpu.VMEM((3, owners, 2, lines, 8, LANES), jnp.float32),
            pltpu.VMEM((3, owners, 2, lines, 8, LANES), jnp.float32),
            pltpu.VMEM((4 * tall, width), jnp.bfloat16),
            pltpu.VMEM((LANES, width), jnp.bfloat16),
            pltpu.VMEM((2, sources, 8, LANES), jnp.float32),
            pltpu.VMEM((2, sources, 8, LANES), jnp.float32),
            dma((7,)),
            dma((quads // SUB, 12)),
            dma((quads // 2 // SUB, 24)),
            dma((3, owners, 2, lines)),
            dma((3, owners, 2, lines)),
            dma((2, sources)),
            dma((2, sources)),
        ],
        compiler_params=pltpu.CompilerParams(
            vmem_limit_bytes=40 * 1024 * 1024, collective_id=0, has_side_effects=True
        ),
    )(*operands)
    return maps.reshape(1, 3, 4, 8 * LANES)


def body(legendre, harmonics, slot_orders, cycle_index):
    owners, sources = lax.axis_size("ma"), lax.axis_size("ell")
    slots, kinds, parts, components, columns = harmonics.shape
    pairs = cycle_index.shape[0]
    fits = (
        (pairs, components, columns, slots) == (2, 4, 4 * LANES, 4 * LANES)
        and owners == 2 * pairs
        and kinds * parts * components == 3 * sources
        and slot_orders.shape[0] * 4 == sources * 8 * LANES
    )
    chosen = packed_body if fits else general_body
    return chosen(legendre, harmonics, slot_orders, cycle_index)


def solution(mesh):
    return jax.shard_map(
        body,
        mesh=mesh,
        in_specs=(P(None, "ma", None, "ell"), P("ma", None, None, None, "ell"), P(), P()),
        out_specs=P("ma", None, None, "ell"),
        check_vma=False,
    )
```

```python
import functools
import math

import jax
import jax.numpy as jnp
import numpy as np
from jax import lax
from jax.experimental import pallas as pl
from jax.experimental.pallas import tpu as pltpu
from jax.sharding import PartitionSpec as P


def column_weights(lower_order, first_column, columns_count, full_width):
    columns = first_column + jnp.arange(columns_count, dtype=jnp.int32)
    boundary = (full_width - 1 - lower_order)[:, None]
    lower_part = (columns[None, :] < boundary).astype(jnp.float32)
    upper_part = ((columns[None, :] >= boundary) & (columns[None, :] < full_width - 1)).astype(
        jnp.float32
    )
    lower_sign = (1 - 2 * (columns[None, :] % 2)).astype(jnp.float32)
    upper_sign = (1 - 2 * ((columns[None, :] + 1 + lower_order[:, None]) % 2)).astype(jnp.float32)
    return jnp.stack(
        [lower_part, lower_part * lower_sign, upper_part, upper_part * upper_sign], axis=1
    )


def spin_fields(plain, plus, minus):
    hemisphere = jnp.array([1.0, -1.0], jnp.float32).reshape(1, 1, 1, 2, 1, 1, 1)
    minus = minus * hemisphere
    temp_real = plain[:, :, :, :, 0]
    temp_imag = plain[:, :, :, :, 1]
    eplus_real = plus[:, :, :, :, 0, 0]
    eplus_imag = plus[:, :, :, :, 0, 1]
    bplus_real = plus[:, :, :, :, 1, 0]
    bplus_imag = plus[:, :, :, :, 1, 1]
    eminus_real = minus[:, :, :, :, 0, 0]
    eminus_imag = minus[:, :, :, :, 0, 1]
    bminus_real = minus[:, :, :, :, 1, 0]
    bminus_imag = minus[:, :, :, :, 1, 1]
    stokes_q_real = -(eplus_real - bminus_imag)
    stokes_q_imag = -(eplus_imag + bminus_real)
    stokes_u_real = -(bplus_real + eminus_imag)
    stokes_u_imag = -(bplus_imag - eminus_real)
    return jnp.stack(
        [
            jnp.stack([temp_real, temp_imag]),
            jnp.stack([stokes_q_real, stokes_q_imag]),
            jnp.stack([stokes_u_real, stokes_u_imag]),
        ]
    )


def place_orders(cycle_orders, lower_all):
    highest = lax.Precision.HIGHEST
    half = lower_all.shape[0]
    width = min(512, half)
    pieces = []
    for start in range(0, half, width):
        targets = start + jnp.arange(width, dtype=jnp.int32)
        onehot = (lower_all[:, None] == targets[None, :]).astype(jnp.float32)
        pieces.append(jnp.einsum("abcdes,sm->abcdem", cycle_orders, onehot, precision=highest))
    placed = jnp.concatenate(pieces, axis=-1)
    return jnp.concatenate([placed[..., 0, :], jnp.flip(placed[..., 1, :], axis=-1)], axis=-1)


def cycle_synthesis(coeff, shift, first_group, group_count):
    highest = lax.Precision.HIGHEST
    cycles_count = coeff.shape[0]
    components = coeff.shape[3]
    orders_count = coeff.shape[-1]
    pixels = 2 * orders_count
    outer = pixels // 128
    groups = orders_count // 128
    orders = jnp.arange(orders_count, dtype=jnp.int32)
    phase = (orders[None, :] * shift[:, None] % (2 * pixels)).astype(jnp.float32) * (
        math.pi / pixels
    )
    factor = jnp.where(orders == 0, 1.0, 2.0).astype(jnp.float32)
    cosine = (jnp.cos(phase) * factor)[:, None, None, :]
    sine = (jnp.sin(phase) * factor)[:, None, None, :]
    real_part = coeff[:, :, 0]
    imag_part = coeff[:, :, 1]
    shifted_real = (real_part * cosine - imag_part * sine).reshape(
        cycles_count, 3, components, groups, 128
    )
    shifted_imag = (real_part * sine + imag_part * cosine).reshape(
        cycles_count, 3, components, groups, 128
    )
    group_ids = jnp.arange(groups, dtype=jnp.int32)
    outer_ids = jnp.arange(outer, dtype=jnp.int32)
    inner_ids = jnp.arange(128, dtype=jnp.int32)
    angle_one = (group_ids[:, None] * outer_ids[None, :] % outer).astype(jnp.float32) * (
        2.0 * math.pi / outer
    )
    cos_one = jnp.cos(angle_one)
    sin_one = jnp.sin(angle_one)
    first_real = jnp.einsum(
        "xyzab,ak->xyzkb", shifted_real, cos_one, precision=highest
    ) - jnp.einsum("xyzab,ak->xyzkb", shifted_imag, sin_one, precision=highest)
    first_imag = jnp.einsum(
        "xyzab,ak->xyzkb", shifted_real, sin_one, precision=highest
    ) + jnp.einsum("xyzab,ak->xyzkb", shifted_imag, cos_one, precision=highest)
    angle_two = (outer_ids[:, None] * inner_ids[None, :] % pixels).astype(jnp.float32) * (
        2.0 * math.pi / pixels
    )
    cos_two = jnp.cos(angle_two)
    sin_two = jnp.sin(angle_two)
    twist_real = first_real * cos_two - first_imag * sin_two
    twist_imag = first_real * sin_two + first_imag * cos_two
    local_ids = first_group + jnp.arange(group_count, dtype=jnp.int32)
    angle_three = (inner_ids[:, None] * local_ids[None, :] % 128).astype(jnp.float32) * (
        2.0 * math.pi / 128
    )
    cos_three = jnp.cos(angle_three)
    sin_three = jnp.sin(angle_three)
    result = jnp.einsum("xyzkb,bq->xyzqk", twist_real, cos_three, precision=highest) - jnp.einsum(
        "xyzkb,bq->xyzqk", twist_imag, sin_three, precision=highest
    )
    return result.reshape(cycles_count, 3, components, group_count * outer)


def general_body(legendre, harmonics, slot_orders, cycle_index):
    ell_count = lax.axis_size("ell")
    slots_here = harmonics.shape[0]
    columns_here = harmonics.shape[-1]
    components = harmonics.shape[3]
    full_width = 2 * slot_orders.shape[0]
    pairs = cycle_index.shape[0]
    lower_here = lax.dynamic_slice_in_dim(
        slot_orders, lax.axis_index("ma") * slots_here, slots_here
    )
    weights = column_weights(
        lower_here, lax.axis_index("ell") * columns_here, columns_here, full_width
    ).astype(jnp.bfloat16)
    packed = harmonics[:, None] * weights[:, :, None, None, None, :]
    plain = jnp.einsum(
        "srj,sqpcj->srqpc", legendre[0], packed[:, :, 0], preferred_element_type=jnp.float32
    )
    plus = jnp.einsum(
        "srj,sqkpcj->srqkpc", legendre[1], packed[:, :, 1:3], preferred_element_type=jnp.float32
    )
    minus = jnp.einsum(
        "srj,sqkpcj->srqkpc", legendre[2], packed[:, :, 1:3], preferred_element_type=jnp.float32
    )
    plain = plain.reshape(slots_here, pairs, 2, 2, 2, components)
    plus = plus.reshape(slots_here, pairs, 2, 2, 2, 2, components)
    minus = minus.reshape(slots_here, pairs, 2, 2, 2, 2, components)
    fields = spin_fields(plain, plus, minus)
    cycle_sums = fields.transpose(5, 3, 0, 1, 6, 4, 2).reshape(
        2 * pairs, 3, 2, components, 2, slots_here
    )
    summed = lax.psum(cycle_sums, "ell")
    cycle_orders = lax.all_to_all(summed, "ma", split_axis=0, concat_axis=5, tiled=True)
    slot_ids = jnp.arange(slot_orders.shape[0], dtype=jnp.int32)
    lower_all = slot_orders[slot_ids]
    coeff = place_orders(cycle_orders, lower_all)
    cycles_here = cycle_orders.shape[0]
    cycle_ids = lax.axis_index("ma") * cycles_here + jnp.arange(cycles_here, dtype=jnp.int32)
    shift = cycle_index[cycle_ids % pairs] % 2
    per_device = 128 // ell_count
    return cycle_synthesis(coeff, shift, lax.axis_index("ell") * per_device, per_device)


LANES = 128
NT = (((1,), (1,)), ((), ()))
SUB = 32


def rotate_sums(group, lane_pair, sub_pair):
    turned = None
    for step in range(4):
        mixed = group[step]
        for pair in range(1, 4):
            mixed = jnp.where(sub_pair == pair, group[(pair + step) % 4], mixed)
        if step == 0:
            turned = mixed
        else:
            mixed = pltpu.roll(mixed, 2 * step, 0)
            turned = jnp.where((sub_pair - lane_pair) % 4 == step, mixed, turned)
    return turned


def fused_kernel(
    width, slots, columns,
    cycle_hbm, orders_hbm, order_rows_hbm, tables_hbm, packed_hbm,
    phase_hbm, first_hbm, twist_hbm, last_hbm, out_ref,
    cycle_ref, orders_ref, rows_ref, table_ref, even_ref, plain_ref,
    phase_ref, first_ref, twist_ref, last_ref,
    spin_part, plain_part, send_ref, held_ref, left_ref, right_ref, pixel_ref, landed_ref,
    small_sem, spin_sem, plain_sem, send_sem, recv_sem, pixel_send, pixel_recv,
):
    owners, sources = lax.axis_size("ma"), lax.axis_size("ell")
    my_owner, my_source = lax.axis_index("ma"), lax.axis_index("ell")
    mesh_ids = pl.DeviceIdType.MESH
    quads = slots // 4
    half = quads // 2
    subs = quads // SUB
    plain_subs = half // SUB

    small = [
        pltpu.make_async_copy(a, b, small_sem.at[i])
        for i, (a, b) in enumerate(
            [
                (orders_hbm, orders_ref),
                (order_rows_hbm, rows_ref),
                (cycle_hbm, cycle_ref),
                (phase_hbm, phase_ref),
                (first_hbm, first_ref),
                (twist_hbm, twist_ref),
                (last_hbm, last_ref),
            ]
        )
    ]

    def spin_copies(sub):
        here = pl.ds(sub * SUB, SUB)
        copies = []
        for g in range(4):
            copies.append((tables_hbm.at[pl.ds(1, 2), g, here], table_ref.at[pl.ds(1, 2), here, :, g]))
            for k in range(2):
                copies.append((packed_hbm.at[g, here, pl.ds(2, 4), k], even_ref.at[here, k, g]))
        return [
            pltpu.make_async_copy(a, b, spin_sem.at[sub, i]) for i, (a, b) in enumerate(copies)
        ]

    def plain_copies(sub):
        copies = []
        to = pl.ds(sub * SUB, SUB)
        for ab in range(2):
            here = pl.ds(ab * half + sub * SUB, SUB)
            for g in range(4):
                copies.append((tables_hbm.at[0, g, here], table_ref.at[0, here, :, g]))
                for k in range(2):
                    copies.append((packed_hbm.at[g, here, pl.ds(0, 2), k], plain_ref.at[to, k, ab, g]))
        return [
            pltpu.make_async_copy(a, b, plain_sem.at[sub, i]) for i, (a, b) in enumerate(copies)
        ]

    def wrapped(place, step, size):
        place = place + step
        return jnp.where(place >= size, place - size, place)

    lines = sources // 2
    my_line, my_side = my_source // 2, my_source % 2
    near_owner = [wrapped(my_owner, i, owners) for i in range(owners)]
    near_line = [wrapped(my_line, i, lines) for i in range(lines)]
    rising = my_line * 2 >= lines
    far_line = [
        wrapped(my_line, jnp.where(rising, i, lines - i), lines) for i in range(1, lines)
    ]
    far_line.append(my_line)
    far_owner = [near_owner[i] for i in (*range(1, owners), 0)]
    others = [
        (owner, line, side)
        for i, line in enumerate(far_line)
        for side in (1 - my_side, my_side)
        for j, owner in enumerate(far_owner)
        if (i, side is my_side, j) != (lines - 1, True, owners - 1)
    ]
    same_owner = [d for d in others if d[0] is near_owner[0]]

    barrier = pltpu.get_barrier_semaphore()

    for owner, line, side in others:
        pl.semaphore_signal(
            barrier, inc=1, device_id=(owner, line * 2 + side), device_id_type=mesh_ids
        )

    small[0].start()
    small[1].start()

    def start_spin(sub, carry):
        for copy in spin_copies(sub):
            copy.start()
        return carry

    def start_plain(sub, carry):
        for copy in plain_copies(sub):
            copy.start()
        return carry

    lax.fori_loop(0, subs, start_spin, 0)
    lax.fori_loop(0, plain_subs, start_plain, 0)
    for copy in small[2:]:
        copy.start()

    lane8 = lax.broadcasted_iota(jnp.int32, (8, LANES), 1)
    sub8 = lax.broadcasted_iota(jnp.int32, (8, LANES), 0)
    lane_low = lax.broadcasted_iota(jnp.int32, (4, LANES), 1) < 64
    small[0].wait()
    small[1].wait()

    def ordered_rows(owner):
        lower = rows_ref[owner]
        turned = pltpu.roll(lower, 64, 1)
        return jnp.concatenate(
            [
                jnp.where(lane_low, lower, width - 1 - turned),
                jnp.where(lane_low, turned, width - 1 - lower),
            ],
            axis=0,
        )

    first_column = my_source * columns
    lane16 = lax.broadcasted_iota(jnp.int32, (16, LANES), 1)
    sub16 = lax.broadcasted_iota(jnp.int32, (16, LANES), 0)
    alternate = (1 - 2 * (lane16 % 2)).astype(jnp.float32).astype(jnp.bfloat16)
    local = (sub16 // 2 % 2) * LANES + lane16
    inside = jnp.where(first_column + local + 2 * LANES < width - 1, 1.0, 0.0).astype(jnp.bfloat16)
    local8 = (sub8 // 2 % 2) * LANES + lane8
    limit = width - 1 - first_column
    sub_pair = sub8 // 2
    flat_even = even_ref.reshape(quads, 2, LANES, LANES)
    flat_plain = plain_ref.reshape(half, 2, LANES, LANES)

    def lower_masks(quad):
        bounds = [limit - orders_ref[my_owner * slots + g * quads + quad] for g in range(4)]
        pairs = [jnp.where(sub8 < 4, bounds[2 * p], bounds[2 * p + 1]) for p in range(2)]
        return [
            jnp.concatenate(
                [jnp.where(local8 + 2 * LANES * k < pair, 1.0, 0.0) for pair in pairs], axis=0
            ).astype(jnp.bfloat16)
            for k in range(2)
        ]

    def weighted(table, quad, masks):
        full = [
            jnp.concatenate([table_ref[table, quad, k, g] for g in range(4)], axis=0)
            for k in range(2)
        ]
        full[1] = full[1] * inside
        low = [full[k] * masks[k] for k in range(2)]
        return [
            jnp.concatenate(pair, axis=1)
            for pair in (full, [v * alternate for v in full], low, [v * alternate for v in low])
        ]

    spin_pair = (lane8 // 32 % 2) * 2 + lane8 // 4 % 2
    plain_pair = (lane8 // 16 % 2) * 2 + lane8 // 4 % 2

    def spin_quad(quad, carry):
        masks = lower_masks(quad)
        left = jnp.concatenate(weighted(1, quad, masks) + weighted(2, quad, masks), axis=0)
        right = jnp.concatenate([flat_even[quad, 0], flat_even[quad, 1]], axis=1)
        product = lax.dot_general(left, right, NT, preferred_element_type=jnp.float32)
        for t in range(2):
            group = []
            for q in range(4):
                at = (t * 4 + q) * 16
                group.append(jnp.where(lane8 < 64, product[at : at + 8], product[at + 8 : at + 16]))
            spin_part[t, pl.ds(pl.multiple_of(quad * 8, 8), 8), :] = rotate_sums(
                group, spin_pair, sub_pair
            )
        return carry

    def plain_octet(octet, carry):
        parts = []
        for ab in range(2):
            quad = octet + ab * half
            parts.append(weighted(0, quad, lower_masks(quad)))
        left = jnp.concatenate([parts[ab][q] for q in range(4) for ab in range(2)], axis=0)
        right = jnp.concatenate([flat_plain[octet, 0], flat_plain[octet, 1]], axis=1)
        product = lax.dot_general(left, right, NT, preferred_element_type=jnp.float32)
        group = []
        for q in range(4):
            chosen = product[q * 32 : q * 32 + 8]
            for g in range(1, 4):
                at = q * 32 + g * 8
                chosen = jnp.where(lane8 // 32 == g, product[at : at + 8], chosen)
            group.append(chosen)
        plain_part[pl.ds(pl.multiple_of(octet * 8, 8), 8), :] = rotate_sums(
            group, plain_pair, sub_pair
        )
        return carry

    def exchange(piece, to, origin):
        owner, line, side = to
        return pltpu.make_async_remote_copy(
            src_ref=send_ref.at[piece, owner, side, line],
            dst_ref=held_ref.at[piece, my_owner, my_side, my_line],
            send_sem=send_sem.at[piece, owner, side, line],
            recv_sem=recv_sem.at[(piece, *origin)],
            device_id=(owner, line * 2 + side),
            device_id_type=mesh_ids,
        )

    def send_piece(piece):
        for device in others:
            exchange(piece, device, (my_owner, my_side, my_line)).start()
        held_ref[piece, my_owner, my_side, my_line] = send_ref[piece, my_owner, my_side, my_line]

    ordered = ordered_rows(my_owner)
    upper_sign = jnp.where(lane8 < 64, 1.0, (1 - 2 * (ordered % 2)).astype(jnp.float32))
    flat_send = send_ref.reshape(3, owners * sources * 8, LANES)

    def by_order(load, south):
        low = load(2 + south)
        return jnp.concatenate([low, load(south) - low], axis=0).T

    def finish_spin(piece):
        first = piece * half * 8
        sign = jnp.where(piece == 0, upper_sign[0:4], upper_sign[4:8])
        for south in range(2):
            for r in range(2):
                plus, minus = (
                    by_order(lambda q: spin_part[t, pl.ds(first + q * 2 + r, half, stride=8), :], south)
                    for t in range(2)
                )
                if south:
                    minus = -minus
                for g in range(4):
                    at = g * 32
                    ep_re, ep_im, bp_re, bp_im = (plus[at + 8 * i : at + 8 * i + 8] for i in range(4))
                    em_re, em_im, bm_re, bm_im = (minus[at + 8 * i : at + 8 * i + 8] for i in range(4))
                    values = (bm_im - ep_re, -(ep_im + bm_re), -(bp_re + em_im), em_re - bp_im)
                    for i, value in enumerate(values):
                        value = value + pltpu.roll(value, 4, 0)
                        if south:
                            value = value * sign[g : g + 1, :]
                        row = ((south * 2 + r) * sources + (i // 2) * 4) * 8 + (i % 2) * 4 + g
                        flat_send[piece, pl.ds(row, 4, stride=8), :] = value[0:4]

    per_piece = half // SUB

    def spin_block(sub, carry):
        for copy in spin_copies(sub):
            copy.wait()
        lax.fori_loop(0, SUB, lambda i, c: spin_quad(sub * SUB + i, c), 0, unroll=SUB)

        @pl.when(lax.rem(sub, per_piece) == per_piece - 1)
        def _():
            finish_spin(lax.div(sub, per_piece))

        @pl.when(sub == per_piece - 1)
        def _():
            pl.semaphore_wait(barrier, len(others))
            send_piece(0)

        return carry

    lax.fori_loop(0, subs, spin_block, 0)
    send_piece(1)

    def plain_block(sub, carry):
        for copy in plain_copies(sub):
            copy.wait()
        return lax.fori_loop(
            0, SUB, lambda i, c: plain_octet(sub * SUB + i, c), carry, unroll=SUB
        )

    lax.fori_loop(0, plain_subs, plain_block, 0)
    for south in range(2):
        for r in range(2):
            turned = by_order(lambda q: plain_part[pl.ds(q * 2 + r, half, stride=8), :], south)
            for k in range(8):
                real, imag = turned[k * 16 : k * 16 + 8], turned[k * 16 + 8 : k * 16 + 16]
                value = jnp.where(
                    sub8 < 4, real + pltpu.roll(real, 4, 0), imag + pltpu.roll(imag, 4, 0)
                )
                if south:
                    value = value * upper_sign[k : k + 1, :]
                row = (south * 2 + r) * sources * 8 + k
                flat_send[2, pl.ds(row, 8, stride=8), :] = value
    send_piece(2)
    lane_rows = lax.broadcasted_iota(jnp.int32, (LANES, LANES), 0)
    for near in range(owners):
        ordered = ordered_rows(lax.rem(my_owner + owners - near, owners))
        for k in range(8):
            at = ((k // 4) * owners + near) * 4 + k % 4
            right_ref[:, at * LANES : (at + 1) * LANES] = jnp.where(
                lane_rows == ordered[k : k + 1, :] % LANES, 1.0, 0.0
            ).astype(jnp.bfloat16)
    for copy in small[2:]:
        copy.wait()

    tall = width // LANES
    tall_ids = lax.broadcasted_iota(jnp.int32, (tall, LANES), 0)

    def split(total):
        high = total.astype(jnp.bfloat16).astype(jnp.float32)
        return high, total - high

    def received(piece, near):
        owner = near_owner[-near % owners]
        for i in range(lines):
            for side in (my_side, 1 - my_side):
                if near or i or side is not my_side:
                    device = (owner, near_line[i], side)
                    exchange(piece, device, (owner, side, near_line[i])).wait_recv()
        total = held_ref[piece, owner, 0, 0] + held_ref[piece, owner, 1, 0]
        for line in range(1, lines):
            total = total + held_ref[piece, owner, 0, line] + held_ref[piece, owner, 1, line]
        return ordered_rows(owner), split(total)

    def place(ordered_row, pieces, row, left_row, at):
        here = tall_ids == ordered_row // LANES
        for i in range(2):
            to = left_row + i * tall
            left_ref[to : to + tall, at * LANES : (at + 1) * LANES] = jnp.where(
                here, pieces[i][row : row + 1, :], 0.0
            ).astype(jnp.bfloat16)

    def place_spin(piece):
        for near in range(owners):
            ordered, pieces = received(piece, near)
            for g in range(4):
                at = (piece * owners + near) * 4 + g
                for part in range(2):
                    place(
                        ordered[piece * 4 + g : piece * 4 + g + 1, :],
                        pieces, part * 4 + g, part * 2 * tall, at,
                    )
        span = pl.ds(piece * owners * 4 * LANES, owners * 4 * LANES)
        return lax.dot_general(
            left_ref[0 : 4 * tall, span], right_ref[:, span], NT, preferred_element_type=jnp.float32
        )

    def joined(placed, at):
        return placed[at : at + tall] + placed[at + tall : at + 2 * tall]

    wide = 2 * tall

    def pixel_copy(which, to, origin):
        source = to[1] * 2 + to[2]
        return pltpu.make_async_remote_copy(
            src_ref=pixel_ref.at[which, source],
            dst_ref=landed_ref.at[which, my_source],
            send_sem=pixel_send.at[which, source],
            recv_sem=pixel_recv.at[which, origin],
            device_id=(my_owner, source),
            device_id_type=mesh_ids,
        )

    def halves(value, axis):
        high = value.astype(jnp.bfloat16)
        low = (value - high.astype(jnp.float32)).astype(jnp.bfloat16)
        return jnp.concatenate([high, low, high], axis=axis)

    def transform(which, real_part, imag_part):
        spectrum = halves(jnp.concatenate([real_part, imag_part], axis=0), 0)
        first = jnp.dot(first_ref[...], spectrum, preferred_element_type=jnp.float32)
        real, imag = first[:wide], first[wide:]
        twisted = jnp.concatenate(
            [
                real * twist_ref[0] - imag * twist_ref[1],
                real * twist_ref[1] + imag * twist_ref[0],
            ],
            axis=1,
        )
        both = lax.dot_general(
            last_ref[...], halves(twisted, 1), NT, preferred_element_type=jnp.float32
        )
        pixels = jnp.concatenate([both[:wide], both[wide:]], axis=1)
        for e in range(sources):
            pixel_ref[which, e] = pixels[e * 8 : e * 8 + 8]
        for device in same_owner:
            pixel_copy(which, device, my_source).start()
        landed_ref[which, my_source] = pixel_ref[which, my_source]

    shifted = cycle_ref[lax.rem(my_owner, cycle_ref.shape[0])] % 2 == 1
    factor = phase_ref[2]
    cosine = jnp.where(shifted, phase_ref[0], factor)
    sine = jnp.where(shifted, phase_ref[1], 0.0)

    placed = place_spin(0)
    placed = placed + place_spin(1)
    real, imag = joined(placed, 0), joined(placed, 2 * tall)
    transform(0, real * cosine - imag * sine, real * sine + imag * cosine)

    placed = None
    for near in range(owners):
        ordered, pieces = received(2, near)
        for k in range(8):
            at = ((k // 4) * owners + near) * 4 + k % 4
            place(ordered[k : k + 1, :], pieces, k, 0, at)
        if near % 2:
            for ab in range(2):
                span = pl.ds((ab * owners + near - 1) * 4 * LANES, 8 * LANES)
                term = lax.dot_general(
                    left_ref[0 : 2 * tall, span], right_ref[:, span], NT, preferred_element_type=jnp.float32
                )
                placed = term if placed is None else placed + term
    value = joined(placed, 0)
    is_real = my_side == 0
    transform(1, value * jnp.where(is_real, cosine, -sine), value * jnp.where(is_real, sine, cosine))
    for piece in range(3):
        for owner, line, side in others:
            exchange(piece, (owner, line, side), (owner, side, line)).wait_send()
    for which in range(2):
        for device in same_owner:
            pixel_copy(which, device, device[1] * 2 + device[2]).wait()
    for c in range(4):
        out_ref[c] = landed_ref[1, 2 * c] + landed_ref[1, 2 * c + 1]
        out_ref[4 + c] = landed_ref[0, 2 * c]
        out_ref[8 + c] = landed_ref[0, 2 * c + 1]


def synthesis_tables(orders_count):
    pixels = 2 * orders_count
    tall = orders_count // LANES
    half = 2 * tall
    orders = np.arange(orders_count).reshape(tall, LANES)
    factor = np.where(orders == 0, 1.0, 2.0)
    angle = orders * (np.pi / pixels)
    phase = np.stack([np.cos(angle) * factor, np.sin(angle) * factor, factor])
    angle = (np.arange(half)[:, None] * np.arange(tall)[None, :] % half) * (2 * np.pi / half)
    first = np.block([[np.cos(angle), -np.sin(angle)], [np.sin(angle), np.cos(angle)]])
    angle = np.arange(half)[:, None] * np.arange(LANES)[None, :] * (2 * np.pi / pixels)
    twist = np.stack([np.cos(angle), np.sin(angle)])
    ids = np.concatenate([np.arange(0, LANES, 2), np.arange(1, LANES, 2)])
    angle = (ids[:, None] * np.arange(LANES)[None, :] % LANES) * (2 * np.pi / LANES)
    last = np.concatenate([np.cos(angle), -np.sin(angle)], axis=1)

    def halved(table):
        high = table.astype(jnp.bfloat16)
        low = (table - high.astype(np.float64)).astype(jnp.bfloat16)
        return jnp.asarray(np.concatenate([high, high, low], axis=1))

    return [
        jnp.asarray(phase, jnp.float32), halved(first), jnp.asarray(twist, jnp.float32), halved(last)
    ]


def packed_body(legendre, harmonics, slot_orders, cycle_index):
    owners, sources = lax.axis_size("ma"), lax.axis_size("ell")
    slots, columns = harmonics.shape[0], harmonics.shape[-1]
    width = 2 * slot_orders.shape[0]
    quads, tall, lines = slots // 4, width // LANES, sources // 2
    tables = (
        legendre.reshape(3, slots, 2, 4, LANES)
        .transpose(0, 1, 3, 2, 4)
        .reshape(3, 4, quads, 2, 4, LANES)
    )
    packed = (
        harmonics.reshape(slots, 3, 2, 4, 4, LANES)
        .transpose(0, 1, 2, 4, 3, 5)
        .reshape(4, quads, 6, 2, 8, LANES)
    )
    constants = synthesis_tables(width)
    operands = [
        pltpu.with_memory_space_constraint(x, pltpu.HBM)
        for x in (
            cycle_index, slot_orders, slot_orders.reshape(owners, 4, LANES), tables, packed, *constants
        )
    ]
    anywhere = pl.BlockSpec(memory_space=pl.ANY)
    dma = pltpu.SemaphoreType.DMA
    maps = pl.pallas_call(
        functools.partial(fused_kernel, width, slots, columns),
        in_specs=[anywhere] * 9,
        out_specs=pl.BlockSpec(memory_space=pltpu.VMEM),
        out_shape=jax.ShapeDtypeStruct((12, 8, LANES), jnp.float32),
        scratch_shapes=[
            pltpu.SMEM(cycle_index.shape, jnp.int32),
            pltpu.SMEM(slot_orders.shape, jnp.int32),
            pltpu.VMEM((owners, 4, LANES), jnp.int32),
            pltpu.VMEM((3, quads, 2, 4, 4, LANES), jnp.bfloat16),
            pltpu.VMEM((quads, 2, 4, 4, 8, LANES), jnp.bfloat16),
            pltpu.VMEM((quads // 2, 2, 2, 4, 2, 8, LANES), jnp.bfloat16),
            *(pltpu.VMEM(c.shape, c.dtype) for c in constants),
            pltpu.VMEM((2, quads * 8, LANES), jnp.float32),
            pltpu.VMEM((quads * 4, LANES), jnp.float32),
            pltpu.VMEM((3, owners, 2, lines, 8, LANES), jnp.float32),
            pltpu.VMEM((3, owners, 2, lines, 8, LANES), jnp.float32),
            pltpu.VMEM((4 * tall, width), jnp.bfloat16),
            pltpu.VMEM((LANES, width), jnp.bfloat16),
            pltpu.VMEM((2, sources, 8, LANES), jnp.float32),
            pltpu.VMEM((2, sources, 8, LANES), jnp.float32),
            dma((7,)),
            dma((quads // SUB, 12)),
            dma((quads // 2 // SUB, 24)),
            dma((3, owners, 2, lines)),
            dma((3, owners, 2, lines)),
            dma((2, sources)),
            dma((2, sources)),
        ],
        compiler_params=pltpu.CompilerParams(
            vmem_limit_bytes=40 * 1024 * 1024, collective_id=0, has_side_effects=True
        ),
    )(*operands)
    return maps.reshape(1, 3, 4, 8 * LANES)


def body(legendre, harmonics, slot_orders, cycle_index):
    owners, sources = lax.axis_size("ma"), lax.axis_size("ell")
    slots, kinds, parts, components, columns = harmonics.shape
    pairs = cycle_index.shape[0]
    fits = (
        (pairs, components, columns, slots) == (2, 4, 4 * LANES, 4 * LANES)
        and owners == 2 * pairs
        and kinds * parts * components == 3 * sources
        and slot_orders.shape[0] * 4 == sources * 8 * LANES
    )
    chosen = packed_body if fits else general_body
    return chosen(legendre, harmonics, slot_orders, cycle_index)


def solution(mesh):
    return jax.shard_map(
        body,
        mesh=mesh,
        in_specs=(P(None, "ma", None, "ell"), P("ma", None, None, None, "ell"), P(), P()),
        out_specs=P("ma", None, None, "ell"),
        check_vma=False,
    )
```
